128 devices in a mesh: row: 32 (over z, y, core), col: 4 (over x).
Axes of the slice: x: 4, y: 4, z: 4, core: 2. Of those that a mesh axis runs over, the one named last changes fastest.
Arguments:
- matrix: float32 [1, 32, 512, 8, 4, 512], P(None, 'row', None, None, 'col'), may hold values from -30 to 30, as said below
Outputs:
- factored: float32 [1, 32, 512, 8, 4, 512], P(None, 'row', None, None, 'col')
The draws below stay inside these ranges and needn't reach their ends.
Inputs may be any that keep to these rules, and one draw needn't show every extreme that they name: matrix is symmetric, positive definite and well conditioned.
All inputs are finite; a program needn't handle non-finite values.
Results may differ from the reference program's by a relative error of at most 0.00013.
Values sent between devices are 32-bit elements; how exact they have to be, the bound alone decides.
A program may use at most 192 MiB of HBM per device.

```python
import jax
import jax.numpy as jnp
from jax import lax

N = 16384
NB = 512
STEPS = 2
TRL = 1
TCL = 8
N_ROW = 32
N_COL = 4


def draw_matrix(key, part):
    gram_cols = 2 * NB
    factor_scale = 2.0 / gram_cols ** 0.5
    key_factor = jax.random.fold_in(key, 11)
    key_diag = jax.random.fold_in(key, 12)
    factor_cols = jax.random.normal(key_factor, (N, gram_cols), jnp.float32) * factor_scale
    diag_values = jax.random.uniform(key_diag, (N,), jnp.float32, 1.0, 2.0)
    scaling = jnp.ones((N,), jnp.float32)
    square = jnp.dot(factor_cols, factor_cols.T, precision=lax.Precision.HIGHEST, preferred_element_type=jnp.float32)
    square = 0.5 * (square + square.T) + jnp.diag(diag_values)
    square = scaling[:, None] * square * scaling[None, :]
    return square.reshape(TRL, N_ROW, NB, TCL, N_COL, NB).astype(jnp.float32)


def setup_inputs(seed: int = 0) -> dict:
    keys = jax.random.split(jax.random.key(seed), 2)
    return {
        "matrix": draw_matrix(jax.random.fold_in(keys[1], 71), 0),
    }


def reference(matrix):
    square = matrix.reshape(N, N)
    for step in range(STEPS):
        begin_at = step * NB
        end_at = begin_at + NB
        diag_factor = jnp.linalg.cholesky(square[begin_at:end_at, begin_at:end_at])
        lower_part = square[end_at:, begin_at:end_at]
        column_panel = jax.scipy.linalg.solve_triangular(diag_factor, lower_part.T, lower=True).T
        trailing = square[end_at:, end_at:] - jnp.dot(column_panel.astype(jnp.float32), column_panel.T.astype(jnp.float32), precision=lax.Precision.HIGHEST, preferred_element_type=jnp.float32)
        square = square.at[end_at:, end_at:].set(trailing)
        square = square.at[end_at:, begin_at:end_at].set(column_panel)
        square = square.at[begin_at:end_at, begin_at:end_at].set(diag_factor)
        square = square.at[begin_at:end_at, end_at:].set(jnp.zeros((NB, N - end_at), jnp.float32))
    return square.reshape(matrix.shape)
```

```python
import functools
import jax
import jax.numpy as jnp
from jax import lax
from jax.experimental import pallas as pl
from jax.experimental.pallas import tpu as pltpu
from jax.sharding import PartitionSpec as P

F32 = jnp.float32
BF = jnp.bfloat16
MESH = pl.DeviceIdType.MESH
NT = (((1,), (1,)), ((), ()))
NN = (((1,), (0,)), ((), ()))
NB = 512
Q = 128


def split(x):
    h=x.astype(BF)
    return h,(x-h.astype(F32)).astype(BF)

def dot3(a,b,dims):
    ah,al=a; bh,bl=b
    d=functools.partial(lax.dot_general,dimension_numbers=dims,preferred_element_type=F32)
    return d(ah,bh)+d(ah,bl)+d(al,bh)

def factor128(D):
    D3=[D[8*i:8*i+8,:] for i in range(16)]
    lane=lax.broadcasted_iota(jnp.int32,(8,128),1)
    sub=lax.broadcasted_iota(jnp.int32,(8,128),0)
    E3=[jnp.where(lane==sub+8*i,1.0,0.0).astype(F32) for i in range(16)]
    def bs(x,k): return jnp.broadcast_to(x[k:k+1,:],(8,128))
    U=[None]*16
    for b in range(16):
        c=8*b
        B={}
        for i in range(b,16):
            for k in range(8):
                B[i,k]=jnp.broadcast_to(D3[i][:,c+k:c+k+1],(8,128))
        g={(k,m):bs(B[b,m],k) for m in range(8) for k in range(m,8)}
        r=[None]*8; s={}
        for m in range(8):
            r[m]=lax.rsqrt(g[m,m])
            for k in range(m+1,8): s[k,m]=g[k,m]*r[m]
            for l in range(m+1,8):
                for k in range(l,8):
                    g[k,l]=g[k,l]-s[k,m]*s[l,m]
        T=D3[b]; Te=E3[b]
        urow=[];erow=[]
        for i in range(b,16):
            mk=[]
            for k in range(8):
                v=B[i,k]
                for m in range(k): v=v-mk[m]*s[k,m]
                mk.append(v*r[k])
            if i==b:
                oU=jnp.zeros((8,128),F32); oE=oU
                for k in range(8):
                    u=bs(T,k)*r[k]; e=bs(Te,k)*r[k]
                    urow.append(u); erow.append(e)
                    oU=jnp.where(sub==k,u,oU); oE=jnp.where(sub==k,e,oE)
                    if k<7:
                        mm=jnp.where(sub>k,mk[k],0.0)
                        T=T-mm*u; Te=Te-mm*e
                U[b]=jnp.where(lane>=sub+c,oU,0.0); E3[b]=oE
            else:
                d=D3[i]; e=E3[i]
                for k in range(8):
                    d=d-mk[k]*urow[k]; e=e-mk[k]*erow[k]
                D3[i]=d; E3[i]=e
    return jnp.concatenate(U,0), jnp.concatenate(E3,0)

def factor_tile(M):
    row=lax.broadcasted_iota(jnp.int32,(1024,128),0)
    def body(k,_):
        c0=pl.multiple_of(k*128,128)
        U,Linv=factor128(M[pl.ds(c0,128),pl.ds(c0,128)])
        P=M[:,pl.ds(c0,128)]
        X=dot3(split(P),split(Linv),NT)
        X=jnp.where(jnp.logical_or(row>=c0+128,row>=512),X,0.0)
        M[:,pl.ds(c0,128)]=X
        M[pl.ds(c0,128),pl.ds(c0,128)]=U.T
        Xl=jnp.where(row[:512]>=c0+128,X[:512],0.0)
        lh,ll=split(Xl)
        for rr in range(4):
            xh,xl=split(X[rr*256:(rr+1)*256])
            M[rr*256:(rr+1)*256,:]-=dot3((xh,xl),(lh,ll),NT)
        return 0
    lax.fori_loop(0,4,body,0)

LEADS = 3
ITEMS = [("L", 0), ("L", 1), ("L", 2)] + [("U", k, s) for s in range(8) for k in range(2)]
NITEM = len(ITEMS)


def place():
    row = lax.axis_index("row")
    return lax.rem(row, 2), lax.rem(row // 2, 4), row // 8, lax.axis_index("col")


def device(y, z, core, x):
    return ((lax.rem(z + 4, 4) * 4 + lax.rem(y + 4, 4)) * 2 + core, lax.rem(x + 4, 4))


def to_tree(t, y, z):
    if t == 0:
        return y, z
    if t == 1:
        return lax.rem(4 - y, 4), lax.rem(4 - z, 4)
    if t == 2:
        return z, y
    return lax.rem(4 - z, 4), lax.rem(4 - y, 4)


def children(t, y, z):
    u, v = to_tree(t, y, z)
    steps = {0: ((1, 0), (0, 1)), 1: ((-1, 0), (0, -1)), 2: ((0, 1), (1, 0)), 3: ((0, -1), (-1, 0))}
    (uy, uz), (vy, vz) = steps[t]
    return (
        ((v == 0) & (u < 3), uy, uz),
        ((u >= 1) & (v < 3), vy, vz),
        ((u == 1) & (v >= 1), -uy, -uz),
    )


def comm_kernel(mat, out, ap_out, buf, ap, load_sem, x_send, x_recv, x_last, t_send, t_recv, p_send, out_sem):
    core, y, z, x = place()
    root = (y == 0) & (z == 0)
    other = 1 - core

    def tile_load(s, dst, sem):
        return [
            pltpu.make_async_copy(mat.at[:, 4 * s + b, 0, :], dst.at[:, pl.ds(128 * b, 128)], sem.at[b])
            for b in range(4)
        ]

    for k in range(2):
        @pl.when(x == k)
        def _():
            for c in tile_load(0, ap.at[k], load_sem.at[8]):
                c.start()

    def item_rows(n):
        return pl.ds(n * NB, NB)

    def u_index(k, s):
        return LEADS + 2 * s + k

    for k in range(2):
        @pl.when(root & (core == k))
        def _():
            for s in range(8):
                for c in tile_load(s, buf.at[item_rows(u_index(k, s))], load_sem.at[s]):
                    c.start()

    barrier = pltpu.get_barrier_semaphore()
    peers = [device(y, z, other, x), device(y, z, core, x + 1), device(y, z, core, x + 3)]
    for dy, dz in ((1, 0), (3, 0), (0, 1), (0, 3)):
        for c in range(2):
            peers.append(device(y + dy, z + dz, c, x))
    for peer in peers:
        pl.semaphore_signal(barrier, inc=1, device_id=peer, device_id_type=MESH)
    pl.semaphore_wait(barrier, len(peers))

    def x_copy(k, part, slot, dx):
        rows = pl.ds(Q * part, Q)
        return pltpu.make_async_remote_copy(
            src_ref=ap.at[k, rows], dst_ref=ap.at[k, rows],
            send_sem=x_send.at[k, part, slot], recv_sem=x_recv.at[k, part],
            device_id=device(y, z, core, x + dx), device_id_type=MESH)

    for k in range(2):
        @pl.when(x == k)
        def _():
            for c in tile_load(0, ap.at[k], load_sem.at[8]):
                c.wait()
            for part in range(4):
                x_copy(k, part, 0, 1).start()
                x_copy(k, part, 1, 3).start()

    def tree_copy(t, n, slot, dy, dz, src=None):
        rows = pl.ds(n * NB + t * Q, Q)
        return pltpu.make_async_remote_copy(
            src_ref=buf.at[rows] if src is None else src.at[pl.ds(t * Q, Q)],
            dst_ref=buf.at[rows],
            send_sem=t_send.at[t, slot], recv_sem=t_recv.at[t, n],
            device_id=device(y + dy, z + dz, t % 2, x), device_id_type=MESH)

    def pair_copy(t, n, src=None):
        rows = pl.ds(n * NB + t * Q, Q)
        return pltpu.make_async_remote_copy(
            src_ref=buf.at[rows] if src is None else src.at[pl.ds(t * Q, Q)],
            dst_ref=buf.at[rows],
            send_sem=p_send.at[t], recv_sem=t_recv.at[t, n],
            device_id=device(y, z, other, x), device_id_type=MESH)

    def x_wait_and_forward():
        for k in range(2):
            for part in range(4):
                far = part // 2
                @pl.when(x != k)
                def _():
                    x_copy(k, part, 0, 1).wait_recv()
                fwd = lax.rem(k + (1 if far == 0 else 3), 4)
                @pl.when(x == fwd)
                def _():
                    x_copy(k, part, 0, 1 if far == 0 else 3).start()

    x_wait_and_forward()

    for k in range(2):
        @pl.when(root & (core == k))
        def _():
            for n, item in enumerate(ITEMS):
                if item[0] == "L":
                    lead = item[1]
                    if (lead == 0) != (k == 0):
                        continue
                    src = ap.at[0 if lead < 2 else 1]
                    for t in range(4):
                        pair_copy(t, n, src).start()
                else:
                    if item[1] != k:
                        continue
                    src = None
                    for c in tile_load(item[2], buf.at[item_rows(n)], load_sem.at[item[2]]):
                        c.wait()
                for t in range(4):
                    (_, dy, dz), _b, _c = children(t, y, z)
                    tree_copy(t, n, 0, dy, dz, src).start()

    def relay(n, _):
        for t in range(4):
            @pl.when(jnp.logical_not(root) & (core == t % 2))
            def _():
                tree_copy(t, n, 0, 0, 1).wait_recv()
                for slot, (cond, dy, dz) in enumerate(children(t, y, z)):
                    @pl.when(cond)
                    def _():
                        tree_copy(t, n, slot, dy, dz).start()
                pair_copy(t, n).start()
        return 0

    def out_copy(n, src):
        return pltpu.make_async_copy(src, out.at[item_rows(n)], out_sem.at[n])

    def drain(n, _):
        for t in range(4):
            @pl.when(jnp.logical_not(root) & (core != t % 2))
            def _():
                pair_copy(t, n).wait_recv()
        @pl.when(jnp.logical_not(root))
        def _():
            out_copy(n, buf.at[item_rows(n)]).start()
        return 0

    def both(n, _):
        relay(n, 0)
        drain(n - 2, 0)
        return 0

    relay(0, 0)
    relay(1, 0)
    lax.fori_loop(2, NITEM, both, 0)
    drain(NITEM - 2, 0)
    drain(NITEM - 1, 0)

    for k in range(2):
        @pl.when(root & (core == k))
        def _():
            for n in range(LEADS):
                if (n == 0) == (k == 0):
                    out_copy(n, ap.at[0 if n < 2 else 1]).start()
                else:
                    for t in range(4):
                        pair_copy(t, n).wait_recv()
                    out_copy(n, buf.at[item_rows(n)]).start()
            for n in range(LEADS):
                out_copy(n, buf.at[item_rows(n)]).wait()

    ap_copy = pltpu.make_async_copy(ap, ap_out, out_sem.at[NITEM])
    ap_copy.start()

    for k in range(2):
        for part in range(4):
            far = part // 2
            fwd = lax.rem(k + (1 if far == 0 else 3), 4)
            @pl.when(x == k)
            def _():
                x_copy(k, part, 0, 1).wait_send()
                x_copy(k, part, 1, 3).wait_send()
            @pl.when(x == fwd)
            def _():
                x_copy(k, part, 0, 1).wait_send()

    def sent(sem, count):
        rows = pl.ds(0, count * Q)
        pltpu.make_async_remote_copy(
            src_ref=buf.at[rows], dst_ref=buf.at[rows], send_sem=sem, recv_sem=t_recv.at[0, 0],
            device_id=device(y, z, other, x), device_id_type=MESH).wait_send()

    for t in range(4):
        @pl.when(jnp.logical_not(root) & (core == t % 2))
        def _():
            for slot, (cond, dy, dz) in enumerate(children(t, y, z)):
                @pl.when(cond)
                def _():
                    sent(t_send.at[t, slot], NITEM)
            sent(p_send.at[t], NITEM)
        for k in range(2):
            @pl.when(root & (core == k))
            def _():
                mine = (1 if k == 0 else 2)
                sent(t_send.at[t, 0], mine + 8)
                sent(p_send.at[t], mine)

    @pl.when(jnp.logical_not(root))
    def _():
        def done(n, _):
            out_copy(n, buf.at[item_rows(n)]).wait()
            return 0
        lax.fori_loop(0, NITEM, done, 0)
    ap_copy.wait()


def gather(mat):
    return pl.pallas_call(
        comm_kernel,
        out_shape=(jax.ShapeDtypeStruct((NITEM * NB, NB), F32), jax.ShapeDtypeStruct((2, NB, NB), F32)),
        in_specs=[pl.BlockSpec(memory_space=pl.ANY)],
        out_specs=(pl.BlockSpec(memory_space=pl.ANY), pl.BlockSpec(memory_space=pl.ANY)),
        scratch_shapes=[
            pltpu.VMEM((NITEM * NB, NB), F32),
            pltpu.VMEM((2, NB, NB), F32),
            pltpu.SemaphoreType.DMA((9, 4)),
            pltpu.SemaphoreType.DMA((2, 4, 2)),
            pltpu.SemaphoreType.DMA((2, 4)),
            pltpu.SemaphoreType.DMA((1,)),
            pltpu.SemaphoreType.DMA((4, 3)),
            pltpu.SemaphoreType.DMA((4, NITEM)),
            pltpu.SemaphoreType.DMA((4,)),
            pltpu.SemaphoreType.DMA((NITEM + 1,)),
        ],
        compiler_params=pltpu.CompilerParams(
            collective_id=0, has_side_effects=True, vmem_limit_bytes=60 * 1024 * 1024),
    )(mat)


def small_kernel(lead, ap, w_out, c_out, m0, m1):
    core, y, z, x = place()
    p = lax.axis_index("row")
    eye = jnp.where(
        lax.broadcasted_iota(jnp.int32, (NB, NB), 0) == lax.broadcasted_iota(jnp.int32, (NB, NB), 1), 1.0, 0.0
    ).astype(F32)
    m0[0:NB, :] = lead[0:NB, :]
    m0[NB:, :] = eye
    factor_tile(m0)
    inv0 = split(m0[NB:, :])
    l10 = dot3(split(lead[NB:2 * NB, :]), inv0, NN)
    l10s = split(l10)
    m1[0:NB, :] = lead[2 * NB:3 * NB, :] - dot3(l10s, l10s, NT)
    m1[NB:, :] = eye
    factor_tile(m1)
    inv1 = split(m1[NB:, :])
    x0 = dot3(split(ap[0]), inv0, NN)
    x1 = dot3(split(ap[1] - dot3(split(x0), l10s, NT)), inv1, NN)
    v = dot3(split(x1), inv1, NT)
    w0 = dot3(split(x0 - dot3(split(v), l10s, NN)), inv0, NT)
    for k, val in ((0, w0), (1, v)):
        h, l = split(val)
        w_out[0, :, k * NB:(k + 1) * NB] = h
        w_out[1, :, k * NB:(k + 1) * NB] = l
    first = jnp.where(p == 0, m0[0:NB, :], jnp.where(p == 1, l10, x0))
    second = jnp.where(p == 0, 0.0, jnp.where(p == 1, m1[0:NB, :], x1))
    c_out[...] = jnp.where(x == 0, first, second)


def small(lead, ap):
    return pl.pallas_call(
        small_kernel,
        out_shape=(jax.ShapeDtypeStruct((2, NB, 2 * NB), BF), jax.ShapeDtypeStruct((NB, NB), F32)),
        in_specs=[pl.BlockSpec((3 * NB, NB), lambda i: (0, 0)), pl.BlockSpec((2, NB, NB), lambda i: (0, 0, 0))],
        out_specs=(pl.BlockSpec((2, NB, 2 * NB), lambda i: (0, 0, 0)), pl.BlockSpec((NB, NB), lambda i: (0, 0))),
        grid=(1,),
        scratch_shapes=[pltpu.VMEM((2 * NB, NB), F32), pltpu.VMEM((2 * NB, NB), F32)],
        compiler_params=pltpu.CompilerParams(vmem_limit_bytes=60 * 1024 * 1024),
    )(lead, ap)


def trail_kernel(mat, g, w, c, out, sbuf, ubuf, obuf, s_sem, u_sem, o_sem):
    x = lax.axis_index("col")
    p = lax.axis_index("row")

    def s_copies(s):
        i = s % 2
        return [pltpu.make_async_copy(mat.at[:, 4 * s + b, 0, :], sbuf.at[i, :, pl.ds(128 * b, 128)], s_sem.at[i, b])
                for b in range(4)]

    def u_copy(s):
        i = s % 2
        return pltpu.make_async_copy(g.at[pl.ds((LEADS + 2 * s) * NB, 2 * NB)], ubuf.at[i], u_sem.at[i])

    def o_copies(s):
        i = s % 2
        return [pltpu.make_async_copy(obuf.at[i, :, pl.ds(128 * b, 128)], out.at[:, 4 * s + b, 0, :], o_sem.at[i, b])
                for b in range(4)]

    def start(s):
        for cp in s_copies(s):
            cp.start()
        u_copy(s).start()

    start(0)
    start(1)
    for s in range(8):
        i = s % 2
        if s >= 2:
            for cp in o_copies(s - 2):
                cp.wait()
        for cp in s_copies(s):
            cp.wait()
        u_copy(s).wait()
        for h in range(2):
            cols = pl.ds(256 * h, 256)
            u = split(ubuf[i, :, cols])
            new = sbuf[i, :, cols] - dot3((w[0], w[1]), u, NN)
            new = jnp.where(p < 2, 0.0, new)
            if s == 0:
                new = jnp.where(x < 2, c[:, cols], new)
            obuf[i, :, cols] = new
        if s + 2 < 8:
            start(s + 2)
        for cp in o_copies(s):
            cp.start()
    for s in (6, 7):
        for cp in o_copies(s):
            cp.wait()


def trail(mat, g, w, c):
    vm = pl.BlockSpec(memory_space=pltpu.VMEM)
    hb = pl.BlockSpec(memory_space=pl.ANY)
    return pl.pallas_call(
        trail_kernel,
        out_shape=jax.ShapeDtypeStruct(mat.shape, F32),
        in_specs=[hb, hb, vm, vm],
        out_specs=hb,
        scratch_shapes=[
            pltpu.VMEM((2, NB, NB), F32), pltpu.VMEM((2, 2 * NB, NB), F32), pltpu.VMEM((2, NB, NB), F32),
            pltpu.SemaphoreType.DMA((2, 4)), pltpu.SemaphoreType.DMA((2,)), pltpu.SemaphoreType.DMA((2, 4)),
        ],
        compiler_params=pltpu.CompilerParams(vmem_limit_bytes=60 * 1024 * 1024),
    )(mat, g, w, c)


def shards(matrix):
    mat = matrix.reshape(NB, 32, 1, 128)
    g, ap = gather(mat)
    w, c = small(g, ap)
    return trail(mat, g, w, c).reshape(matrix.shape)


def solution(mesh):
    spec = P(None, "row", None, None, "col", None)
    return jax.shard_map(shards, mesh=mesh, in_specs=(spec,), out_specs=spec, check_vma=False)
```

```python
import functools
import jax
import jax.numpy as jnp
from jax import lax
from jax.experimental import pallas as pl
from jax.experimental.pallas import tpu as pltpu
from jax.sharding import PartitionSpec as P

F32 = jnp.float32
BF = jnp.bfloat16
MESH = pl.DeviceIdType.MESH
NT = (((1,), (1,)), ((), ()))
NN = (((1,), (0,)), ((), ()))
NB = 512
Q = 128


def split(x):
    h=x.astype(BF)
    return h,(x-h.astype(F32)).astype(BF)

def dot3(a,b,dims):
    ah,al=a; bh,bl=b
    d=functools.partial(lax.dot_general,dimension_numbers=dims,preferred_element_type=F32)
    return d(ah,bh)+d(ah,bl)+d(al,bh)

def factor128(D):
    D3 = [D[8 * i:8 * i + 8, :] for i in range(16)]
    lane = lax.broadcasted_iota(jnp.int32, (8, 128), 1)
    sub = lax.broadcasted_iota(jnp.int32, (8, 128), 0)
    E3 = [jnp.where(lane == sub + 8 * i, 1.0, 0.0).astype(F32) for i in range(16)]
    zero = jnp.zeros((8, 128), F32)

    def bs(x, k):
        return jnp.take_along_axis(x, jnp.full((8, 128), k, jnp.int32), axis=0)

    U = [None] * 16
    for b in range(16):
        c = 8 * b
        B = {}
        for i in range(b, 16):
            for k in range(8):
                B[i, k] = jnp.broadcast_to(D3[i][:, c + k:c + k + 1], (8, 128))
        g = {(k, m): bs(B[b, m], k) for m in range(8) for k in range(m, 8)}
        r = [None] * 8
        s = {}
        for m in range(8):
            r[m] = lax.rsqrt(g[m, m])
            for k in range(m + 1, 8):
                s[k, m] = g[k, m] * r[m]
            for l in range(m + 1, 8):
                for k in range(l, 8):
                    g[k, l] = g[k, l] - s[k, m] * s[l, m]
        urow, erow = [], []
        for i in range(b, 16):
            mk = []
            for k in range(8):
                v = B[i, k]
                for m in range(k):
                    v = v - mk[m] * s[k, m]
                mk.append(v * r[k])
            d, e = D3[i], E3[i]
            if i == b:
                ou, oe = zero, zero
                for k in range(8):
                    u, w = bs(d, k) * r[k], bs(e, k) * r[k]
                    urow.append(u)
                    erow.append(w)
                    ou, oe = jnp.where(sub == k, u, ou), jnp.where(sub == k, w, oe)
                    if k < 7:
                        mm = jnp.where(sub > k, mk[k], 0.0)
                        d, e = d - mm * u, e - mm * w
                U[b] = jnp.where(lane >= sub + c, ou, 0.0)
                E3[b] = oe
            else:
                for k in range(8):
                    d, e = d - mk[k] * urow[k], e - mk[k] * erow[k]
                D3[i], E3[i] = d, e
    return jnp.concatenate(U, 0), jnp.concatenate(E3, 0)


def factor_tile(M):
    row = lax.broadcasted_iota(jnp.int32, (512, 128), 0)

    def body(k, _):
        c0 = pl.multiple_of(k * 128, 128)
        cols = pl.ds(c0, 128)
        U, Linv = factor128(M[cols, cols])
        live = pl.ds(pl.multiple_of(c0 + 128, 128), 512)
        X = dot3(split(M[live, cols]), split(Linv), NT)
        M[live, cols] = X
        M[cols, cols] = U.T
        lead = split(jnp.where(row >= c0 + 128, M[0:512, cols], 0.0))
        M[0:512, cols] = jnp.where(row >= c0, M[0:512, cols], 0.0)
        xh, xl = split(X)
        for h in range(2):
            r = slice(256 * h, 256 * h + 256)
            part = pl.ds(pl.multiple_of(c0 + 128 + 256 * h, 128), 256)
            M[part, :] -= dot3((xh[r], xl[r]), lead, NT)
        return 0

    lax.fori_loop(0, 4, body, 0)

LEADS = 3
NITEM = LEADS + 16
ORDER = [3, 4, 0, 5, 6, 1, 2] + list(range(7, NITEM))
DEEP = 6
PIECES = 2
R = Q // PIECES


def place():
    row = lax.axis_index("row")
    return lax.rem(row, 2), lax.rem(row // 2, 4), row // 8, lax.axis_index("col")


def device(y, z, core, x):
    return ((lax.rem(z + 4, 4) * 4 + lax.rem(y + 4, 4)) * 2 + core, lax.rem(x + 4, 4))


def to_tree(t, y, z):
    if t == 0:
        return y, z
    if t == 1:
        return lax.rem(4 - y, 4), lax.rem(4 - z, 4)
    if t == 2:
        return z, y
    return lax.rem(4 - z, 4), lax.rem(4 - y, 4)


def depth(t, y, z):
    u, v = to_tree(t, y, z)
    return jnp.where((u == 0) & (v > 0), 2 + v, u + v)


def at_step(i):
    head = jnp.where(i < 2, i + 3, jnp.where(i < 3, 0, jnp.where(i < 5, i + 2, i - 4)))
    return jnp.where(i < 7, head, i)


def children(t, y, z):
    u, v = to_tree(t, y, z)
    steps = {0: ((1, 0), (0, 1)), 1: ((-1, 0), (0, -1)), 2: ((0, 1), (1, 0)), 3: ((0, -1), (-1, 0))}
    (uy, uz), (vy, vz) = steps[t]
    return (
        ((v == 0) & (u < 3), uy, uz),
        ((u >= 1) & (v < 3), vy, vz),
        ((u == 1) & (v >= 1), -uy, -uz),
    )


def front_kernel(mat, out, w_out, c_out, buf, ap, m0, m1, wbuf, cbuf,
                 load_sem, x_send, x_recv, t_send, t_recv, p_send, lead_recv, u_recv, out_sem, w_sem, w_recv):
    core, y, z, x = place()
    root = (y == 0) & (z == 0)
    inner = jnp.logical_not(root)
    other = 1 - core

    def tile_load(s, dst, sem):
        return [
            pltpu.make_async_copy(mat.at[:, 4 * s + b, 0, :], dst.at[:, pl.ds(128 * b, 128)], sem.at[b])
            for b in range(4)
        ]

    def item_rows(n):
        return pl.ds(n * NB, NB)

    def item(k, s):
        return LEADS + 2 * s + k

    for k in range(2):
        for c in range(2):
            @pl.when((x == k) & (core == c))
            def _():
                for cp in tile_load(0, ap.at[c, k], load_sem.at[8]):
                    cp.start()
    for k in range(2):
        @pl.when(root & (core == k))
        def _():
            for s in range(8):
                for cp in tile_load(s, buf.at[item_rows(item(k, s))], load_sem.at[s]):
                    cp.start()

    barrier = pltpu.get_barrier_semaphore()
    peers = [device(y, z, other, x)]
    for c in range(2):
        peers += [device(y, z, c, x + 1), device(y, z, c, x + 3)]
        for dy, dz in ((1, 0), (3, 0), (0, 1), (0, 3)):
            peers.append(device(y + dy, z + dz, c, x))
    for peer in peers:
        pl.semaphore_signal(barrier, inc=1, device_id=peer, device_id_type=MESH)
    pl.semaphore_wait(barrier, len(peers))

    def x_copy(c, k, part, slot, dx):
        rows = pl.ds(Q * part, Q)
        return pltpu.make_async_remote_copy(
            src_ref=ap.at[c, k, rows], dst_ref=ap.at[c, k, rows],
            send_sem=x_send.at[c, k, part, slot], recv_sem=x_recv.at[c, k, part],
            device_id=device(y, z, 0, x + dx), device_id_type=MESH)

    for k in range(2):
        for c in range(2):
            @pl.when((x == k) & (core == c))
            def _():
                for cp in tile_load(0, ap.at[c, k], load_sem.at[8]):
                    cp.wait()
                for part in range(4):
                    x_copy(c, k, part, 0, 1).start()
                    x_copy(c, k, 3 - part, 1, 3).start()
                if c == 1:
                    for part in range(4):
                        x_copy(c, k, part, 2, 0).start()

    def x_far(k, part):
        return lax.rem(k + (1 if part < 2 else 3), 4), (1 if part < 2 else 3)

    def x_wait(c, k, part):
        x_copy(c, k, part, 0, 1).wait_recv()

    def x_forward(c, k):
        for part in (0, 3, 1, 2):
            fwd, dx = x_far(k, part)
            @pl.when(x == fwd)
            def _():
                x_wait(c, k, part)
                x_copy(c, k, part, 0, dx).start()

    def x_rest(c, k, part):
        fwd, _dx = x_far(k, part)
        away = (x != fwd) if c == 1 else (x != k) & (x != fwd)
        @pl.when(away)
        def _():
            x_wait(c, k, part)

    def piece(t, n, h):
        return pl.ds(pl.multiple_of(n * NB + t * Q + h * R, 8), R)

    def tree_copy(t, n, h, slot, dy, dz, src=None):
        rows = piece(t, n, h)
        return pltpu.make_async_remote_copy(
            src_ref=buf.at[rows] if src is None else src.at[pl.ds(t * Q + h * R, R)],
            dst_ref=buf.at[rows],
            send_sem=t_send.at[t, slot], recv_sem=t_recv.at[t, n * PIECES + h],
            device_id=device(y + dy, z + dz, 1, x), device_id_type=MESH)

    def lead_copy(t, n, h):
        rows = piece(t, n, h)
        return pltpu.make_async_remote_copy(
            src_ref=buf.at[rows], dst_ref=buf.at[rows],
            send_sem=p_send.at[t], recv_sem=lead_recv.at[n],
            device_id=device(y, z, other, x), device_id_type=MESH)

    def out_piece(t, n, h):
        return pl.ds(pl.multiple_of((n - LEADS) * NB + t * Q + h * R, 8), R)

    def u_copy(t, n, h):
        return pltpu.make_async_remote_copy(
            src_ref=buf.at[piece(t, n, h)], dst_ref=out.at[out_piece(t, n, h)],
            send_sem=p_send.at[t], recv_sem=u_recv.at[n - LEADS],
            device_id=device(y, z, other, x), device_id_type=MESH)

    def own_copy(t, n, h):
        return pltpu.make_async_copy(buf.at[piece(t, n, h)], out.at[out_piece(t, n, h)], out_sem.at[n - LEADS])

    for k in range(2):
        @pl.when(root & (core == k))
        def _():
            for n in ORDER:
                if n < LEADS:
                    if k == 1:
                        continue
                    c, kk = ((0, 0), (1, 0), (1, 1))[n]
                    src = ap.at[c, kk]
                    x_forward(c, kk)
                else:
                    if (n - LEADS) % 2 != k:
                        continue
                    c, src = None, None
                    s = (n - LEADS) // 2
                    for cp in tile_load(s, buf.at[item_rows(n)], load_sem.at[s]):
                        cp.wait()
                for t in range(4):
                    if c is not None:
                        x_rest(c, kk, t)
                    (_, dy, dz), _b, _c = children(t, y, z)
                    for h in range(PIECES):
                        tree_copy(t, n, h, 0, dy, dz, src).start()
            if k == 0:
                x_forward(0, 1)

    @pl.when(inner & (core == 0))
    def _():
        for k in range(2):
            for c in range(2):
                x_forward(c, k)

    skews = [(7 * depth(t, y, z)) // 3 for t in range(4)]
    LAST = (7 * DEEP) // 3

    def relay(step, _):
        for t in range(4):
            i = step - skews[t]
            @pl.when((i >= 0) & (i < PIECES * NITEM))
            def _():
                n, h = at_step(i // PIECES), lax.rem(i, PIECES)
                tree_copy(t, n, h, 0, 0, 1).wait_recv()
                for slot, (cond, dy, dz) in enumerate(children(t, y, z)):
                    @pl.when(cond)
                    def _():
                        tree_copy(t, n, h, slot, dy, dz).start()
                @pl.when(n < LEADS)
                def _():
                    lead_copy(t, n, h).start()
                @pl.when(n >= LEADS)
                def _():
                    u_copy(t, n, h).start()
                    own_copy(t, n, h).start()
        return 0

    @pl.when(inner & (core == 1))
    def _():
        lax.fori_loop(0, PIECES * NITEM + LAST, relay, 0)

    def lead_wait(n):
        rows = item_rows(n)
        pltpu.make_async_remote_copy(
            src_ref=buf.at[rows], dst_ref=buf.at[rows], send_sem=p_send.at[0], recv_sem=lead_recv.at[n],
            device_id=device(y, z, other, x), device_id_type=MESH).wait_recv()

    def lead_into(dst, n):
        c, k = ((0, 0), (1, 0), (1, 1))[n]
        @pl.when(root)
        def _():
            dst[0:NB, :] = ap[c, k]
        @pl.when(inner)
        def _():
            lead_wait(n)
            dst[0:NB, :] = buf[n * NB:(n + 1) * NB, :]

    @pl.when(core == 0)
    def _():
        eye = jnp.where(
            lax.broadcasted_iota(jnp.int32, (NB, NB), 0) == lax.broadcasted_iota(jnp.int32, (NB, NB), 1), 1.0, 0.0
        ).astype(F32)
        lead_into(m0, 0)
        m0[NB:, :] = eye
        factor_tile(m0)
        inv0 = split(m0[NB:, :])
        lead_into(cbuf.at[0], 1)
        l10 = dot3(split(cbuf[0]), inv0, NN)
        cbuf[0] = l10
        l10s = split(l10)
        lead_into(m1, 2)
        m1[0:NB, :] -= dot3(l10s, l10s, NT)
        m1[NB:, :] = eye
        factor_tile(m1)
        for k in range(2):
            for part in range(4):
                for c in range(2):
                    fwd, _dx = x_far(k, part)
                    here = (x == k) if c == 0 else (x < 0)
                    taken = here | (x == fwd) if (c, k) == (0, 1) else here | (x == fwd) | root
                    @pl.when(jnp.logical_not(taken))
                    def _():
                        x_wait(c, k, part)
        inv0, inv1 = split(m0[NB:, :]), split(m1[NB:, :])
        l10s = split(cbuf[0])
        for c in (1, 0):
            x0 = dot3(split(ap[c, 0]), inv0, NN)
            x1 = dot3(split(ap[c, 1] - dot3(split(x0), l10s, NT)), inv1, NN)
            v = dot3(split(x1), inv1, NT)
            wbuf[c, :, NB:] = v
            wbuf[c, :, :NB] = dot3(split(x0 - dot3(split(v), l10s, NN)), inv0, NT)
            if c == 1:
                first = jnp.where(root, cbuf[0], x0)
                second = jnp.where(root, m1[0:NB, :], x1)
            else:
                first = jnp.where(root, m0[0:NB, :], x0)
                second = jnp.where(root, 0.0, x1)
            cbuf[c] = jnp.where(x == 0, first, second)

    def results():
        pair = device(y, z, other, x)
        return [
            pltpu.make_async_remote_copy(
                src_ref=src, dst_ref=dst, send_sem=w_sem.at[i], recv_sem=w_recv.at[i],
                device_id=pair, device_id_type=MESH)
            for i, (src, dst) in enumerate(((wbuf.at[1], w_out), (cbuf.at[1], c_out)))
        ]

    @pl.when(core == 0)
    def _():
        own = [pltpu.make_async_copy(wbuf.at[0], w_out, w_sem.at[2]),
               pltpu.make_async_copy(cbuf.at[0], c_out, w_sem.at[3])]
        for cp in results() + own:
            cp.start()
        for cp in results():
            cp.wait_send()
        for cp in own:
            cp.wait()
        @pl.when(inner)
        def _():
            for i in range(16):
                rows = pl.ds(i * NB, NB)
                pltpu.make_async_remote_copy(
                    src_ref=out.at[rows], dst_ref=out.at[rows], send_sem=p_send.at[0], recv_sem=u_recv.at[i],
                    device_id=device(y, z, other, x), device_id_type=MESH).wait_recv()

    @pl.when(core == 1)
    def _():
        @pl.when(inner)
        def _():
            for i in range(16):
                pltpu.make_async_copy(
                    buf.at[pl.ds((LEADS + i) * NB, NB)], out.at[pl.ds(i * NB, NB)], out_sem.at[i]).wait()
        for cp in results():
            cp.wait_recv()

    for c in range(2):
        for k in range(2):
            for part in range(4):
                fwd, _dx = x_far(k, part)
                @pl.when((x == k) & (core == c))
                def _():
                    x_copy(c, k, part, 0, 1).wait_send()
                    x_copy(c, k, part, 1, 3).wait_send()
                    if c == 1:
                        x_copy(c, k, part, 2, 0).wait_send()
                @pl.when((x == fwd) & (core == 0))
                def _():
                    x_copy(c, k, part, 0, 1).wait_send()

    def sent(sem, count):
        rows = pl.ds(0, count * Q)
        pltpu.make_async_remote_copy(
            src_ref=buf.at[rows], dst_ref=buf.at[rows], send_sem=sem, recv_sem=t_recv.at[0, 0],
            device_id=device(y, z, other, x), device_id_type=MESH).wait_send()

    for t in range(4):
        @pl.when(inner & (core == 1))
        def _():
            for slot, (cond, dy, dz) in enumerate(children(t, y, z)):
                @pl.when(cond)
                def _():
                    sent(t_send.at[t, slot], NITEM)
            sent(p_send.at[t], NITEM)
        for k in range(2):
            @pl.when(root & (core == k))
            def _():
                sent(t_send.at[t, 0], 8 + (LEADS if k == 0 else 0))


def front(mat):
    hb = pl.BlockSpec(memory_space=pl.ANY)
    dma = pltpu.SemaphoreType.DMA
    return pl.pallas_call(
        front_kernel,
        out_shape=(
            jax.ShapeDtypeStruct((16 * NB, NB), F32),
            jax.ShapeDtypeStruct((NB, 2 * NB), F32),
            jax.ShapeDtypeStruct((NB, NB), F32),
        ),
        in_specs=[hb],
        out_specs=(hb, hb, hb),
        scratch_shapes=[
            pltpu.VMEM((NITEM * NB, NB), F32),
            pltpu.VMEM((2, 2, NB, NB), F32),
            pltpu.VMEM((2 * NB, NB), F32),
            pltpu.VMEM((2 * NB, NB), F32),
            pltpu.VMEM((2, NB, 2 * NB), F32),
            pltpu.VMEM((2, NB, NB), F32),
            dma((9, 4)), dma((2, 2, 4, 3)), dma((2, 2, 4)), dma((4, 3)), dma((4, NITEM * PIECES)),
            dma((4,)), dma((LEADS,)), dma((16,)), dma((16,)), dma((4,)), dma((2,)),
        ],
        compiler_params=pltpu.CompilerParams(
            collective_id=0, has_side_effects=True, vmem_limit_bytes=63 * 1024 * 1024),
    )(mat)


def trail_kernel(mat, g, w, c, out, whl, sbuf, ubuf, obuf, s_sem, u_sem, o_sem):
    x = lax.axis_index("col")
    p = lax.axis_index("row")

    def s_copies(s):
        i = s % 2
        return [pltpu.make_async_copy(mat.at[:, 4 * s + b, 0, :], sbuf.at[i, :, pl.ds(128 * b, 128)], s_sem.at[i, b])
                for b in range(4)]

    def u_copy(s):
        i = s % 2
        return pltpu.make_async_copy(g.at[pl.ds(2 * s * NB, 2 * NB)], ubuf.at[i], u_sem.at[i])

    def o_copies(s):
        i = s % 2
        return [pltpu.make_async_copy(obuf.at[i, :, pl.ds(128 * b, 128)], out.at[:, 4 * s + b, 0, :], o_sem.at[i, b])
                for b in range(4)]

    def start(s):
        for cp in s_copies(s):
            cp.start()
        u_copy(s).start()

    start(0)
    start(1)
    whl[0], whl[1] = split(w[...])
    for s in range(8):
        i = s % 2
        if s >= 2:
            for cp in o_copies(s - 2):
                cp.wait()
        for cp in s_copies(s):
            cp.wait()
        u_copy(s).wait()
        for h in range(2):
            cols = pl.ds(256 * h, 256)
            u = split(ubuf[i, :, cols])
            new = sbuf[i, :, cols] - dot3((whl[0], whl[1]), u, NN)
            new = jnp.where(p < 2, 0.0, new)
            if s == 0:
                new = jnp.where(x < 2, c[:, cols], new)
            obuf[i, :, cols] = new
        if s + 2 < 8:
            start(s + 2)
        for cp in o_copies(s):
            cp.start()
    for s in (6, 7):
        for cp in o_copies(s):
            cp.wait()


def trail(mat, g, w, c):
    vm = pl.BlockSpec(memory_space=pltpu.VMEM)
    hb = pl.BlockSpec(memory_space=pl.ANY)
    return pl.pallas_call(
        trail_kernel,
        out_shape=jax.ShapeDtypeStruct(mat.shape, F32),
        in_specs=[hb, hb, vm, vm],
        out_specs=hb,
        scratch_shapes=[
            pltpu.VMEM((2, NB, 2 * NB), BF),
            pltpu.VMEM((2, NB, NB), F32), pltpu.VMEM((2, 2 * NB, NB), F32), pltpu.VMEM((2, NB, NB), F32),
            pltpu.SemaphoreType.DMA((2, 4)), pltpu.SemaphoreType.DMA((2,)), pltpu.SemaphoreType.DMA((2, 4)),
        ],
        compiler_params=pltpu.CompilerParams(vmem_limit_bytes=60 * 1024 * 1024),
    )(mat, g, w, c)


def shards(matrix):
    mat = matrix.reshape(NB, 32, 1, 128)
    u, w, c = front(mat)
    return trail(mat, u, w, c).reshape(matrix.shape)


def solution(mesh):
    spec = P(None, "row", None, None, "col", None)
    return jax.shard_map(shards, mesh=mesh, in_specs=(spec,), out_specs=spec, check_vma=False)
```

```python
import functools
import jax
import jax.numpy as jnp
from jax import lax
from jax.experimental import pallas as pl
from jax.experimental.pallas import tpu as pltpu
from jax.sharding import PartitionSpec as P

F32 = jnp.float32
BF = jnp.bfloat16
MESH = pl.DeviceIdType.MESH
NT = (((1,), (1,)), ((), ()))
NN = (((1,), (0,)), ((), ()))
NB = 512
Q = 128


def split(x):
    h=x.astype(BF)
    return h,(x-h.astype(F32)).astype(BF)

def dot3(a,b,dims):
    ah,al=a; bh,bl=b
    d=functools.partial(lax.dot_general,dimension_numbers=dims,preferred_element_type=F32)
    return d(ah,bh)+d(ah,bl)+d(al,bh)

def factor128(D):
    D3 = [D[8 * i:8 * i + 8, :] for i in range(16)]
    lane = lax.broadcasted_iota(jnp.int32, (8, 128), 1)
    sub = lax.broadcasted_iota(jnp.int32, (8, 128), 0)
    E3 = [jnp.where(lane == sub + 8 * i, 1.0, 0.0).astype(F32) for i in range(16)]
    zero = jnp.zeros((8, 128), F32)

    def bs(x, k):
        return jnp.take_along_axis(x, jnp.full((8, 128), k, jnp.int32), axis=0)

    U = [None] * 16
    for b in range(16):
        c = 8 * b
        B = {}
        for i in range(b, 16):
            for k in range(8):
                B[i, k] = jnp.broadcast_to(D3[i][:, c + k:c + k + 1], (8, 128))
        g = {(k, m): bs(B[b, m], k) for m in range(8) for k in range(m, 8)}
        r = [None] * 8
        s = {}
        for m in range(8):
            r[m] = lax.rsqrt(g[m, m])
            for k in range(m + 1, 8):
                s[k, m] = g[k, m] * r[m]
            for l in range(m + 1, 8):
                for k in range(l, 8):
                    g[k, l] = g[k, l] - s[k, m] * s[l, m]
        urow, erow = [], []
        for i in range(b, 16):
            mk = []
            for k in range(8):
                v = B[i, k]
                for m in range(k):
                    v = v - mk[m] * s[k, m]
                mk.append(v * r[k])
            d, e = D3[i], E3[i]
            if i == b:
                ou, oe = zero, zero
                for k in range(8):
                    u, w = bs(d, k) * r[k], bs(e, k) * r[k]
                    urow.append(u)
                    erow.append(w)
                    ou, oe = jnp.where(sub == k, u, ou), jnp.where(sub == k, w, oe)
                    if k < 7:
                        mm = jnp.where(sub > k, mk[k], 0.0)
                        d, e = d - mm * u, e - mm * w
                U[b] = jnp.where(lane >= sub + c, ou, 0.0)
                E3[b] = oe
            else:
                for k in range(8):
                    d, e = d - mk[k] * urow[k], e - mk[k] * erow[k]
                D3[i], E3[i] = d, e
    return jnp.concatenate(U, 0), jnp.concatenate(E3, 0)


def factor_tile(M):
    row = lax.broadcasted_iota(jnp.int32, (512, 128), 0)

    def body(k, _):
        c0 = pl.multiple_of(k * 128, 128)
        cols = pl.ds(c0, 128)
        U, Linv = factor128(M[cols, cols])
        live = pl.ds(pl.multiple_of(c0 + 128, 128), 512)
        X = dot3(split(M[live, cols]), split(Linv), NT)
        M[live, cols] = X
        M[cols, cols] = U.T
        lead = split(jnp.where(row >= c0 + 128, M[0:512, cols], 0.0))
        M[0:512, cols] = jnp.where(row >= c0, M[0:512, cols], 0.0)
        xh, xl = split(X)
        for h in range(2):
            r = slice(256 * h, 256 * h + 256)
            part = pl.ds(pl.multiple_of(c0 + 128 + 256 * h, 128), 256)
            M[part, :] -= dot3((xh[r], xl[r]), lead, NT)
        return 0

    lax.fori_loop(0, 4, body, 0)

LEADS = 3
NITEM = LEADS + 16
ORDER = [3, 4, 5, 6, 0, 8, 7, 10, 9, 12, 11, 14, 1, 16, 2, 18, 13, 15, 17]
DEEP = 6
PIECES = 4
R = Q // PIECES


def place():
    row = lax.axis_index("row")
    return lax.rem(row, 2), lax.rem(row // 2, 4), row // 8, lax.axis_index("col")


def device(y, z, core, x):
    return ((lax.rem(z + 4, 4) * 4 + lax.rem(y + 4, 4)) * 2 + core, lax.rem(x + 4, 4))


def to_tree(t, y, z):
    if t == 0:
        return y, z
    if t == 1:
        return lax.rem(4 - y, 4), lax.rem(4 - z, 4)
    if t == 2:
        return z, y
    return lax.rem(4 - z, 4), lax.rem(4 - y, 4)


def depth(t, y, z):
    u, v = to_tree(t, y, z)
    return jnp.where((u == 0) & (v > 0), 2 + v, u + v)


def at_step(i):
    j = i // 2
    odd = 4 + 2 * j
    even = jnp.where(j < 2, 3 + 2 * j, jnp.where(j < 3, 0, jnp.where(j < 6, 1 + 2 * j, jnp.where(j < 7, 1, 2))))
    return jnp.where(i >= 16, 13 + 2 * (i - 16), jnp.where(lax.rem(i, 2) == 1, odd, even))


def children(t, y, z):
    u, v = to_tree(t, y, z)
    steps = {0: ((1, 0), (0, 1)), 1: ((-1, 0), (0, -1)), 2: ((0, 1), (1, 0)), 3: ((0, -1), (-1, 0))}
    (uy, uz), (vy, vz) = steps[t]
    return (
        ((v == 0) & (u < 3), uy, uz),
        ((u >= 1) & (v < 3), vy, vz),
        ((u == 1) & (v >= 1), -uy, -uz),
    )


def front_kernel(mat, out, fac, ap_out, top, buf, ap, m0, m1, tmp,
                 load_sem, pace, x_send, x_recv, t_send, t_recv, p_send, lead_recv, u_recv, out_sem, f_send, f_recv, f_own):
    core, y, z, x = place()
    root = (y == 0) & (z == 0)
    inner = jnp.logical_not(root)
    other = 1 - core

    def tile_load(s, dst, sem):
        return [
            pltpu.make_async_copy(mat.at[:, 4 * s + b, 0, :], dst.at[:, pl.ds(128 * b, 128)], sem.at[b])
            for b in range(4)
        ]

    def item_rows(n):
        return pl.ds(n * NB, NB)

    def item(k, s):
        return LEADS + 2 * s + k

    for k in range(2):
        for c in range(2):
            @pl.when((x == k) & (core == c))
            def _():
                for cp in tile_load(0, ap.at[c, k], load_sem.at[8]):
                    cp.start()
    for k in range(2):
        @pl.when(root & (core == k))
        def _():
            for s in range(8):
                for cp in tile_load(s, buf.at[item_rows(item(k, s))], load_sem.at[s]):
                    cp.start()

    barrier = pltpu.get_barrier_semaphore()
    peers = [device(y, z, other, x)]
    for c in range(2):
        peers += [device(y, z, c, x + 1), device(y, z, c, x + 3)]
        for dy, dz in ((1, 0), (3, 0), (0, 1), (0, 3)):
            peers.append(device(y + dy, z + dz, c, x))
    for peer in peers:
        pl.semaphore_signal(barrier, inc=1, device_id=peer, device_id_type=MESH)
    pl.semaphore_wait(barrier, len(peers))

    def x_copy(c, k, part, slot, dx):
        rows = pl.ds(Q * part, Q)
        return pltpu.make_async_remote_copy(
            src_ref=ap.at[c, k, rows], dst_ref=ap.at[c, k, rows],
            send_sem=x_send.at[c, k, part, slot], recv_sem=x_recv.at[c, k, part],
            device_id=device(y, z, 0, x + dx), device_id_type=MESH)

    for k in range(2):
        for c in range(2):
            @pl.when((x == k) & (core == c))
            def _():
                for cp in tile_load(0, ap.at[c, k], load_sem.at[8]):
                    cp.wait()
                if c == 1:
                    for part in range(4):
                        x_copy(c, k, part, 2, 0).start()
                @pl.when(inner if (c, k) != (0, 0) else core == 0)
                def _():
                    for part in range(4):
                        x_copy(c, k, part, 0, 1).start()
                        x_copy(c, k, 3 - part, 1, 3).start()

    def x_far(k, part):
        return lax.rem(k + (1 if part < 2 else 3), 4), (1 if part < 2 else 3)

    def x_wait(c, k, part):
        x_copy(c, k, part, 0, 1).wait_recv()

    def x_forward(c, k):
        for part in (0, 3, 1, 2):
            fwd, dx = x_far(k, part)
            @pl.when(x == fwd)
            def _():
                x_wait(c, k, part)
                x_copy(c, k, part, 0, dx).start()

    def root_send(k):
        @pl.when(x == k)
        def _():
            for part in range(4):
                x_wait(1, k, part)
            for part in range(4):
                x_copy(1, k, part, 0, 1).start()
                x_copy(1, k, 3 - part, 1, 3).start()

    def root_rest(c, k, part):
        fwd, _dx = x_far(k, part)
        @pl.when((x != k) & (x != fwd))
        def _():
            x_wait(c, k, part)

    def piece(t, n, h):
        return pl.ds(pl.multiple_of(n * NB + t * Q + h * R, 8), R)

    def tree_copy(t, n, h, slot, dy, dz, src=None):
        rows = piece(t, n, h)
        return pltpu.make_async_remote_copy(
            src_ref=buf.at[rows] if src is None else src.at[pl.ds(t * Q + h * R, R)],
            dst_ref=buf.at[rows],
            send_sem=t_send.at[t, slot], recv_sem=t_recv.at[t, n * PIECES + h],
            device_id=device(y + dy, z + dz, 1, x), device_id_type=MESH)

    def lead_copy(t, n, h):
        rows = piece(t, n, h)
        return pltpu.make_async_remote_copy(
            src_ref=buf.at[rows], dst_ref=buf.at[rows],
            send_sem=p_send.at[t], recv_sem=lead_recv.at[n],
            device_id=device(y, z, other, x), device_id_type=MESH)

    def out_piece(t, n, h):
        return pl.ds(pl.multiple_of((n - LEADS) * NB + t * Q + h * R, 8), R)

    def u_copy(t, n, h):
        return pltpu.make_async_remote_copy(
            src_ref=buf.at[piece(t, n, h)], dst_ref=out.at[out_piece(t, n, h)],
            send_sem=p_send.at[t], recv_sem=u_recv.at[n - LEADS],
            device_id=device(y, z, other, x), device_id_type=MESH)

    def own_copy(t, n, h):
        return pltpu.make_async_copy(buf.at[piece(t, n, h)], out.at[out_piece(t, n, h)], out_sem.at[n - LEADS])

    for k in range(2):
        @pl.when(root & (core == k))
        def _():
            for n in ORDER:
                if n < LEADS:
                    if k == 1:
                        continue
                    c, kk = ((0, 0), (1, 0), (1, 1))[n]
                    src = ap.at[c, kk]
                    if n == 1:
                        x_forward(1, 0)
                        x_forward(1, 1)
                else:
                    if (n - LEADS) % 2 != k:
                        continue
                    c, src = None, None
                    s = (n - LEADS) // 2
                    if k == 1 and s > 0:
                        pl.semaphore_wait(pace, 1)
                    for cp in tile_load(s, buf.at[item_rows(n)], load_sem.at[s]):
                        cp.wait()
                for t in range(4):
                    if c is not None:
                        root_rest(c, kk, t)
                    (_, dy, dz), _b, _c = children(t, y, z)
                    for h in range(PIECES):
                        tree_copy(t, n, h, 0, dy, dz, src).start()
                if k == 0 and n == 3:
                    root_send(0)
                if k == 0 and n == 5:
                    x_forward(0, 0)
                    root_send(1)
                if k == 0 and n in ORDER[:14:2]:
                    pl.semaphore_signal(pace, inc=1, device_id=device(y, z, other, x), device_id_type=MESH)

    @pl.when(inner & (core == 0))
    def _():
        for k in range(2):
            for c in range(2):
                x_forward(c, k)

    skews = [4 * depth(t, y, z) for t in range(4)]
    LAST = 4 * DEEP

    def relay(step, _):
        for t in range(4):
            i = step - skews[t]
            @pl.when((i >= 0) & (i < PIECES * NITEM))
            def _():
                n, h = at_step(i // PIECES), lax.rem(i, PIECES)
                tree_copy(t, n, h, 0, 0, 1).wait_recv()
                for slot, (cond, dy, dz) in enumerate(children(t, y, z)):
                    @pl.when(cond)
                    def _():
                        tree_copy(t, n, h, slot, dy, dz).start()
                @pl.when(n < LEADS)
                def _():
                    lead_copy(t, n, h).start()
                @pl.when(n >= LEADS)
                def _():
                    u_copy(t, n, h).start()
                    own_copy(t, n, h).start()
        return 0

    @pl.when(inner & (core == 1))
    def _():
        lax.fori_loop(0, PIECES * NITEM + LAST, relay, 0)

    def lead_wait(n):
        rows = item_rows(n)
        pltpu.make_async_remote_copy(
            src_ref=buf.at[rows], dst_ref=buf.at[rows], send_sem=p_send.at[0], recv_sem=lead_recv.at[n],
            device_id=device(y, z, other, x), device_id_type=MESH).wait_recv()

    def lead_into(dst, n):
        c, k = ((0, 0), (1, 0), (1, 1))[n]
        @pl.when(root)
        def _():
            dst[0:NB, :] = ap[c, k]
        @pl.when(inner)
        def _():
            lead_wait(n)
            dst[0:NB, :] = buf[n * NB:(n + 1) * NB, :]

    def result(i, c):
        return (
            (ap.at[c, 0], ap_out.at[0]), (ap.at[c, 1], ap_out.at[1]),
            (m0.at[pl.ds(NB, NB)], fac.at[0]), (tmp, fac.at[1]), (m1.at[pl.ds(NB, NB)], fac.at[2]),
            (tmp, top), (m1.at[pl.ds(0, NB)], top),
        )[i]

    def hand(i):
        src, dst = result(i, 1)
        sem = min(i, 5)
        return pltpu.make_async_remote_copy(
            src_ref=src, dst_ref=dst, send_sem=f_send.at[sem], recv_sem=f_recv.at[sem],
            device_id=device(y, z, other, x), device_id_type=MESH)

    def keep(i):
        src, dst = result(i, 0)
        return pltpu.make_async_copy(src, dst, f_own.at[i])

    @pl.when(core == 0)
    def _():
        eye = jnp.where(
            lax.broadcasted_iota(jnp.int32, (NB, NB), 0) == lax.broadcasted_iota(jnp.int32, (NB, NB), 1), 1.0, 0.0
        ).astype(F32)
        lead_into(m0, 0)
        m0[NB:, :] = eye
        factor_tile(m0)
        inv0 = split(m0[NB:, :])
        lead_into(tmp, 1)
        l10 = dot3(split(tmp[...]), inv0, NN)
        tmp[...] = l10
        l10s = split(l10)
        lead_into(m1, 2)
        m1[0:NB, :] -= dot3(l10s, l10s, NT)
        m1[NB:, :] = eye
        for k in range(2):
            for part in range(4):
                for c in range(2):
                    fwd, _dx = x_far(k, part)
                    here = (x == k) if c == 0 else (x < 0)
                    @pl.when(jnp.logical_not(here | (x == fwd) | root))
                    def _():
                        x_wait(c, k, part)
        for i in range(4):
            hand(i).start()
            keep(i).start()
        factor_tile(m1)
        hand(4).start()
        keep(4).start()
        @pl.when(root)
        def _():
            pltpu.make_async_copy(m0.at[pl.ds(0, NB)], top, f_own.at[5]).start()
            @pl.when(x == 0)
            def _():
                hand(5).start()
            @pl.when(x != 0)
            def _():
                hand(6).start()
        for i in range(5):
            hand(i).wait_send()
            keep(i).wait()
        @pl.when(root)
        def _():
            pltpu.make_async_copy(m0.at[pl.ds(0, NB)], top, f_own.at[5]).wait()
            hand(5).wait_send()

    @pl.when((core == 0) & inner)
    def _():
        for i in range(16):
            rows = pl.ds(i * NB, NB)
            pltpu.make_async_remote_copy(
                src_ref=out.at[rows], dst_ref=out.at[rows], send_sem=p_send.at[0], recv_sem=u_recv.at[i],
                device_id=device(y, z, other, x), device_id_type=MESH).wait_recv()

    @pl.when(core == 1)
    def _():
        @pl.when(inner)
        def _():
            for i in range(16):
                pltpu.make_async_copy(
                    buf.at[pl.ds((LEADS + i) * NB, NB)], out.at[pl.ds(i * NB, NB)], out_sem.at[i]).wait()
        for i in range(5):
            hand(i).wait_recv()
        @pl.when(root)
        def _():
            hand(5).wait_recv()

    for c in range(2):
        for k in range(2):
            for part in range(4):
                fwd, _dx = x_far(k, part)
                sender = jnp.where(root, (core == 0) & ((c, k) != (0, 1)), core == c)
                @pl.when((x == k) & sender)
                def _():
                    x_copy(c, k, part, 0, 1).wait_send()
                    x_copy(c, k, part, 1, 3).wait_send()
                if c == 1:
                    @pl.when((x == k) & (core == 1))
                    def _():
                        x_copy(c, k, part, 2, 0).wait_send()
                passed = (x == fwd) & (core == 0)
                @pl.when(passed & inner if (c, k) == (0, 1) else passed)
                def _():
                    x_copy(c, k, part, 0, 1).wait_send()

    def sent(sem, count):
        rows = pl.ds(0, count * Q)
        pltpu.make_async_remote_copy(
            src_ref=buf.at[rows], dst_ref=buf.at[rows], send_sem=sem, recv_sem=t_recv.at[0, 0],
            device_id=device(y, z, other, x), device_id_type=MESH).wait_send()

    for t in range(4):
        @pl.when(inner & (core == 1))
        def _():
            for slot, (cond, dy, dz) in enumerate(children(t, y, z)):
                @pl.when(cond)
                def _():
                    sent(t_send.at[t, slot], NITEM)
            sent(p_send.at[t], NITEM)
        for k in range(2):
            @pl.when(root & (core == k))
            def _():
                sent(t_send.at[t, 0], 8 + (LEADS if k == 0 else 0))


def front(mat):
    hb = pl.BlockSpec(memory_space=pl.ANY)
    dma = pltpu.SemaphoreType.DMA
    return pl.pallas_call(
        front_kernel,
        out_shape=(
            jax.ShapeDtypeStruct((16 * NB, NB), F32),
            jax.ShapeDtypeStruct((3, NB, NB), F32),
            jax.ShapeDtypeStruct((2, NB, NB), F32),
            jax.ShapeDtypeStruct((NB, NB), F32),
        ),
        in_specs=[hb],
        out_specs=(hb, hb, hb, hb),
        scratch_shapes=[
            pltpu.VMEM((NITEM * NB, NB), F32),
            pltpu.VMEM((2, 2, NB, NB), F32),
            pltpu.VMEM((2 * NB, NB), F32),
            pltpu.VMEM((2 * NB, NB), F32),
            pltpu.VMEM((NB, NB), F32),
            dma((9, 4)), pltpu.SemaphoreType.REGULAR, dma((2, 2, 4, 3)), dma((2, 2, 4)), dma((4, 3)), dma((4, NITEM * PIECES)),
            dma((4,)), dma((LEADS,)), dma((16,)), dma((16,)), dma((6,)), dma((6,)), dma((6,)),
        ],
        compiler_params=pltpu.CompilerParams(
            collective_id=0, has_side_effects=True, vmem_limit_bytes=63 * 1024 * 1024),
    )(mat)


def tri(a, inv):
    low = tuple(v[:, :256] for v in a)
    return jnp.concatenate([
        dot3(low, tuple(v[:256, :256] for v in inv), NN),
        dot3(a, tuple(v[:, 256:] for v in inv), NN)], 1)


def tri_t(a, inv):
    high = tuple(v[:, 256:] for v in a)
    return jnp.concatenate([
        dot3(a, tuple(v[:256, :] for v in inv), NT),
        dot3(high, tuple(v[256:, 256:] for v in inv), NT)], 1)


def trail_kernel(mat, u, fac, ap, top, out, fv, av, tv, whl, sbuf, ubuf, obuf, f_sem, s_sem, u_sem, o_sem):
    x = lax.axis_index("col")
    p = lax.axis_index("row")
    OUT = obuf.shape[0]

    def s_copies(s):
        return [pltpu.make_async_copy(mat.at[:, 4 * s + b, 0, :], sbuf.at[s, :, pl.ds(128 * b, 128)], s_sem.at[s, b])
                for b in range(4)]

    def u_copy(s):
        return pltpu.make_async_copy(u.at[pl.ds(2 * s * NB, 2 * NB)], ubuf.at[s], u_sem.at[s])

    def o_copies(s):
        i = s % OUT
        return [pltpu.make_async_copy(obuf.at[i, :, pl.ds(128 * b, 128)], out.at[:, 4 * s + b, 0, :], o_sem.at[i, b])
                for b in range(4)]

    first = [
        pltpu.make_async_copy(ap.at[0], av.at[0], f_sem.at[0]),
        pltpu.make_async_copy(fac.at[0], fv.at[0], f_sem.at[1]),
        pltpu.make_async_copy(ap.at[1], av.at[1], f_sem.at[2]),
        pltpu.make_async_copy(fac.at[1], fv.at[1], f_sem.at[3]),
        pltpu.make_async_copy(fac.at[2], fv.at[2], f_sem.at[4]),
        pltpu.make_async_copy(top, tv, f_sem.at[5]),
    ]
    for cp in first:
        cp.start()
    for s in range(8):
        u_copy(s).start()
        for cp in s_copies(s):
            cp.start()

    first[0].wait()
    first[1].wait()
    inv0 = split(fv[0])
    x0 = tri(split(av[0]), inv0)
    first[2].wait()
    first[3].wait()
    l10 = split(fv[1])
    rest = av[1] - dot3(split(x0), l10, NT)
    first[4].wait()
    inv1 = split(fv[2])
    x1 = tri(split(rest), inv1)
    v = tri_t(split(x1), inv1)
    vs = split(v)
    ws = split(tri_t(split(x0 - dot3(vs, l10, NN)), inv0))
    for i in range(2):
        whl[i, :, :NB] = ws[i]
        whl[i, :, NB:] = vs[i]
    first[5].wait()
    own = jnp.where((p == 0) & (x > 0), 0.0, tv[...])
    av[0] = jnp.where(p < 2, own, jnp.where(x == 0, x0, x1))

    for s in range(8):
        if s >= OUT:
            for cp in o_copies(s - OUT):
                cp.wait()
        u_copy(s).wait()
        for cp in s_copies(s):
            cp.wait()
        for h in range(2):
            cols = pl.ds(256 * h, 256)
            part = split(ubuf[s, :, cols])
            new = sbuf[s, :, cols] - dot3((whl[0], whl[1]), part, NN)
            new = jnp.where(p < 2, 0.0, new)
            if s == 0:
                new = jnp.where(x < 2, av[0, :, cols], new)
            obuf[s % OUT, :, cols] = new
        for cp in o_copies(s):
            cp.start()
    for s in range(8 - OUT, 8):
        for cp in o_copies(s):
            cp.wait()


def trail(mat, u, fac, ap, top):
    hb = pl.BlockSpec(memory_space=pl.ANY)
    dma = pltpu.SemaphoreType.DMA
    return pl.pallas_call(
        trail_kernel,
        out_shape=jax.ShapeDtypeStruct(mat.shape, F32),
        in_specs=[hb] * 5,
        out_specs=hb,
        scratch_shapes=[
            pltpu.VMEM((3, NB, NB), F32), pltpu.VMEM((2, NB, NB), F32), pltpu.VMEM((NB, NB), F32),
            pltpu.VMEM((2, NB, 2 * NB), BF),
            pltpu.VMEM((8, NB, NB), F32), pltpu.VMEM((8, 2 * NB, NB), F32), pltpu.VMEM((3, NB, NB), F32),
            dma((6,)), dma((8, 4)), dma((8,)), dma((3, 4)),
        ],
        compiler_params=pltpu.CompilerParams(vmem_limit_bytes=63 * 1024 * 1024),
    )(mat, u, fac, ap, top)


def shards(matrix):
    mat = matrix.reshape(NB, 32, 1, 128)
    return trail(mat, *front(mat)).reshape(matrix.shape)


def solution(mesh):
    spec = P(None, "row", None, None, "col", None)
    return jax.shard_map(shards, mesh=mesh, in_specs=(spec,), out_specs=spec, check_vma=False)
```

```python
import functools
import jax
import jax.numpy as jnp
from jax import lax
from jax.experimental import pallas as pl
from jax.experimental.pallas import tpu as pltpu
from jax.sharding import PartitionSpec as P

F32 = jnp.float32
BF = jnp.bfloat16
MESH = pl.DeviceIdType.MESH
NT = (((1,), (1,)), ((), ()))
NN = (((1,), (0,)), ((), ()))
NB = 512
Q = 128


def split(x):
    h=x.astype(BF)
    return h,(x-h.astype(F32)).astype(BF)

def dot3(a,b,dims):
    ah,al=a; bh,bl=b
    d=functools.partial(lax.dot_general,dimension_numbers=dims,preferred_element_type=F32)
    return d(ah,bh)+d(ah,bl)+d(al,bh)

def factor128(D):
    D3 = [D[8 * i:8 * i + 8, :] for i in range(16)]
    lane = lax.broadcasted_iota(jnp.int32, (8, 128), 1)
    sub = lax.broadcasted_iota(jnp.int32, (8, 128), 0)
    E3 = [jnp.where(lane == sub + 8 * i, 1.0, 0.0).astype(F32) for i in range(16)]
    zero = jnp.zeros((8, 128), F32)

    def bs(x, k):
        return jnp.take_along_axis(x, jnp.full((8, 128), k, jnp.int32), axis=0)

    U = [None] * 16
    for b in range(16):
        c = 8 * b
        B = {}
        for i in range(b, 16):
            for k in range(8):
                B[i, k] = jnp.broadcast_to(D3[i][:, c + k:c + k + 1], (8, 128))
        g = {(k, m): bs(B[b, m], k) for m in range(8) for k in range(m, 8)}
        r = [None] * 8
        s = {}
        for m in range(8):
            r[m] = lax.rsqrt(g[m, m])
            for k in range(m + 1, 8):
                s[k, m] = g[k, m] * r[m]
            for l in range(m + 1, 8):
                for k in range(l, 8):
                    g[k, l] = g[k, l] - s[k, m] * s[l, m]
        urow, erow = [], []
        for i in range(b, 16):
            mk = []
            for k in range(8):
                v = B[i, k]
                for m in range(k):
                    v = v - mk[m] * s[k, m]
                mk.append(v * r[k])
            d, e = D3[i], E3[i]
            if i == b:
                ou, oe = zero, zero
                for k in range(8):
                    u, w = bs(d, k) * r[k], bs(e, k) * r[k]
                    urow.append(u)
                    erow.append(w)
                    ou, oe = jnp.where(sub == k, u, ou), jnp.where(sub == k, w, oe)
                    if k < 7:
                        mm = jnp.where(sub > k, mk[k], 0.0)
                        d, e = d - mm * u, e - mm * w
                U[b] = jnp.where(lane >= sub + c, ou, 0.0)
                E3[b] = oe
            else:
                for k in range(8):
                    d, e = d - mk[k] * urow[k], e - mk[k] * erow[k]
                D3[i], E3[i] = d, e
    return jnp.concatenate(U, 0), jnp.concatenate(E3, 0)


def factor_tile(M):
    row = lax.broadcasted_iota(jnp.int32, (512, 128), 0)

    def body(k, _):
        c0 = pl.multiple_of(k * 128, 128)
        cols = pl.ds(c0, 128)
        U, Linv = factor128(M[cols, cols])
        live = pl.ds(pl.multiple_of(c0 + 128, 128), 512)
        X = dot3(split(M[live, cols]), split(Linv), NT)
        M[live, cols] = X
        M[cols, cols] = U.T
        below = M[0:512, cols]
        M[0:512, cols] = jnp.where(row >= c0, below, 0.0)
        xs = split(X)
        for j in range(3):
            @pl.when(k == j)
            def _():
                right = slice(128 * (j + 1), 512)
                lead = split(below[right])
                for h in range(2):
                    r = slice(256 * h, 256 * h + 256)
                    start = 128 * (j + 1) + 256 * h
                    M[start:start + 256, right] -= dot3(tuple(v[r] for v in xs), lead, NT)
        return 0

    lax.fori_loop(0, 4, body, 0)

LEADS = 3
NITEM = LEADS + 16
EVEN = [3, 5, 7, 1, 2, 9, 11, 13, 15, 17]
ODD = [4, 6, 8, 10, 12, 14, 16, 18]
DEEP = 6
PIECES = 4
GATE = 12
R = Q // PIECES


def place():
    row = lax.axis_index("row")
    return lax.rem(row, 2), lax.rem(row // 2, 4), row // 8, lax.axis_index("col")


def device(y, z, core, x):
    return ((lax.rem(z + 4, 4) * 4 + lax.rem(y + 4, 4)) * 2 + core, lax.rem(x + 4, 4))


def to_tree(t, y, z):
    if t == 0:
        return y, z
    if t == 1:
        return lax.rem(4 - y, 4), lax.rem(4 - z, 4)
    if t == 2:
        return z, y
    return lax.rem(4 - z, 4), lax.rem(4 - y, 4)


def depth(t, y, z):
    u, v = to_tree(t, y, z)
    return jnp.where((u == 0) & (v > 0), 2 + v, u + v)


def at_step(i, x):
    j = i // 2
    at = jnp.where(x == 0, 0, 1)
    even = jnp.where(j < 2, jnp.where(j == at, 0, 3), jnp.where(j < 4, 2 * j + 1, jnp.where(j < 6, j - 3, 2 * j - 3)))
    return jnp.where(i >= 16, 13 + 2 * (i - 16), jnp.where(lax.rem(i, 2) == 1, 4 + 2 * j, even))


def children(t, y, z):
    u, v = to_tree(t, y, z)
    steps = {0: ((1, 0), (0, 1)), 1: ((-1, 0), (0, -1)), 2: ((0, 1), (1, 0)), 3: ((0, -1), (-1, 0))}
    (uy, uz), (vy, vz) = steps[t]
    return (
        ((v == 0) & (u < 3), uy, uz),
        ((u >= 1) & (v < 3), vy, vz),
        ((u == 1) & (v >= 1), -uy, -uz),
    )


def front_kernel(mat, out, fac, ap_out, top, buf, ap, m0, m1, tmp,
                 load_sem, pace, c_send, x_send, x_recv, t_send, t_recv, p_send, lead_recv, u_recv, out_sem, f_send, f_recv, f_own):
    core, y, z, x = place()
    root = (y == 0) & (z == 0)
    inner = jnp.logical_not(root)
    firsts = [depth(t, y, z) == 1 for t in range(4)]
    child = firsts[0] | firsts[1] | firsts[2] | firsts[3]
    other = 1 - core

    def tile_load(s, dst, sem):
        return [
            pltpu.make_async_copy(mat.at[:, 4 * s + b, 0, :], dst.at[:, pl.ds(128 * b, 128)], sem.at[b])
            for b in range(4)
        ]

    def item_rows(n):
        return pl.ds(n * NB, NB)

    def item(k, s):
        return LEADS + 2 * s + k

    for k in range(2):
        for c in range(2):
            @pl.when((x == k) & (core == c))
            def _():
                for cp in tile_load(0, ap.at[c, k], load_sem.at[8]):
                    cp.start()
    def row_loads(tiles):
        for k in range(2):
            @pl.when(root & (core == k))
            def _():
                for s in tiles:
                    for cp in tile_load(s, buf.at[item_rows(item(k, s))], load_sem.at[s]):
                        cp.start()

    row_loads((0,))

    barrier = pltpu.get_barrier_semaphore()
    peers = [device(y, z, other, x)]
    for c in range(2):
        peers += [device(y, z, c, x + d) for d in (1, 2, 3)]
        for dy, dz in ((1, 0), (3, 0), (0, 1), (0, 3)):
            peers.append(device(y + dy, z + dz, c, x))
    for peer in peers:
        pl.semaphore_signal(barrier, inc=1, device_id=peer, device_id_type=MESH)
    pl.semaphore_wait(barrier, len(peers))
    row_loads(range(1, 8))

    def x_copy(c, k, part, slot, dx):
        rows = pl.ds(Q * part, Q)
        return pltpu.make_async_remote_copy(
            src_ref=ap.at[c, k, rows], dst_ref=ap.at[c, k, rows],
            send_sem=x_send.at[c, k, part, slot], recv_sem=x_recv.at[c, k, part],
            device_id=device(y, z, 0, x + dx), device_id_type=MESH)

    def x_sends(c, k):
        for part in range(4):
            x_copy(c, k, part, 0, 1).start()
            x_copy(c, k, 3 - part, 1, 3).start()

    for k in range(2):
        for c in range(2):
            @pl.when((x == k) & (core == c))
            def _():
                for cp in tile_load(0, ap.at[c, k], load_sem.at[8]):
                    cp.wait()
                if c == 1:
                    for part in range(4):
                        x_copy(c, k, part, 2, 0).start()
                away = inner & jnp.logical_not(child)
                @pl.when(away)
                def _():
                    x_sends(c, k)

    def x_far(k, part):
        return lax.rem(k + (1 if part < 2 else 3), 4), (1 if part < 2 else 3)

    def x_wait(c, k, part):
        x_copy(c, k, part, 0, 1).wait_recv()

    def x_forward(c, k):
        for part in (0, 3, 1, 2):
            fwd, dx = x_far(k, part)
            @pl.when(x == fwd)
            def _():
                x_wait(c, k, part)
                x_copy(c, k, part, 0, dx).start()

    def root_send(k):
        @pl.when(x == k)
        def _():
            for part in range(4):
                x_wait(1, k, part)
            x_sends(1, k)

    def root_rest(c, k, part):
        fwd, _dx = x_far(k, part)
        @pl.when((x != k) & (x != fwd))
        def _():
            x_wait(c, k, part)

    def piece(t, n, h):
        return pl.ds(pl.multiple_of(n * NB + t * Q + h * R, 8), R)

    def tree_copy(t, n, h, slot, dy, dz, src=None):
        rows = piece(t, n, h)
        return pltpu.make_async_remote_copy(
            src_ref=buf.at[rows] if src is None else src.at[pl.ds(t * Q + h * R, R)],
            dst_ref=buf.at[rows],
            send_sem=t_send.at[t, slot], recv_sem=t_recv.at[t, n * PIECES + h],
            device_id=device(y + dy, z + dz, 1, x), device_id_type=MESH)

    def lead_copy(t, n, h):
        rows = piece(t, n, h)
        return pltpu.make_async_remote_copy(
            src_ref=buf.at[rows], dst_ref=buf.at[rows],
            send_sem=p_send.at[t], recv_sem=lead_recv.at[n],
            device_id=device(y, z, other, x), device_id_type=MESH)

    def out_piece(t, n, h):
        return pl.ds(pl.multiple_of((n - LEADS) * NB + t * Q + h * R, 8), R)

    def u_copy(t, n, h):
        return pltpu.make_async_remote_copy(
            src_ref=buf.at[piece(t, n, h)], dst_ref=out.at[out_piece(t, n, h)],
            send_sem=p_send.at[t], recv_sem=u_recv.at[n - LEADS],
            device_id=device(y, z, other, x), device_id_type=MESH)

    def own_copy(t, n, h):
        return pltpu.make_async_copy(buf.at[piece(t, n, h)], out.at[out_piece(t, n, h)], out_sem.at[n - LEADS])

    def root_tree(n, src):
        for t in range(4):
            (_, dy, dz), _b, _c = children(t, y, z)
            for h in range(PIECES):
                tree_copy(t, n, h, 0, dy, dz, src).start()

    @pl.when(root & (core == 0))
    def _():
        @pl.when(x == 0)
        def _():
            root_tree(0, ap.at[0, 0])
        for k in range(2):
            root_send(k)
        @pl.when(x == 0)
        def _():
            x_sends(0, 0)
        for n in EVEN:
            if n < LEADS:
                kk = n - 1
                if n == 1:
                    x_forward(1, 0)
                    x_forward(1, 1)
                for t in range(4):
                    root_rest(1, kk, t)
                root_tree(n, ap.at[1, kk])
            else:
                for cp in tile_load((n - LEADS) // 2, buf.at[item_rows(n)], load_sem.at[(n - LEADS) // 2]):
                    cp.wait()
                root_tree(n, None)
            if n == 9:
                x_forward(0, 0)
            if n in EVEN[:7]:
                pl.semaphore_signal(pace, inc=1, device_id=device(y, z, other, x), device_id_type=MESH)
        for t in range(4):
            root_rest(0, 0, t)

    @pl.when(root & (core == 1))
    def _():
        for n in ODD:
            for cp in tile_load((n - LEADS) // 2, buf.at[item_rows(n)], load_sem.at[(n - LEADS) // 2]):
                cp.wait()
            if n > 4:
                pl.semaphore_wait(pace, 1)
            root_tree(n, None)

    def cross_copy(t, h, slot):
        rows = piece(t, 0, h)
        return pltpu.make_async_remote_copy(
            src_ref=buf.at[rows], dst_ref=buf.at[rows],
            send_sem=c_send.at[slot], recv_sem=t_recv.at[t, h],
            device_id=device(y, z, 1, x + slot + 1), device_id_type=MESH)

    @pl.when(child & (core == 0) & (x < 2))
    def _():
        pl.semaphore_wait(pace, 1)
        for k in range(2):
            @pl.when(x == k)
            def _():
                x_sends(0, k)

    @pl.when(inner & (core == 0))
    def _():
        for k in range(2):
            for c in range(2):
                x_forward(c, k)

    skews = [4 * depth(t, y, z) for t in range(4)]
    LAST = 4 * DEEP

    def relay(step, _):
        for t in range(4):
            i = step - skews[t]
            @pl.when((i >= 0) & (i < PIECES * NITEM))
            def _():
                n, h = at_step(i // PIECES, x), lax.rem(i, PIECES)
                tree_copy(t, n, h, 0, 0, 1).wait_recv()
                for slot, (cond, dy, dz) in enumerate(children(t, y, z)):
                    @pl.when(cond)
                    def _():
                        tree_copy(t, n, h, slot, dy, dz).start()
                @pl.when((n == 0) & (x == 0) & firsts[t])
                def _():
                    for slot in (0, 2, 1):
                        cross_copy(t, h, slot).start()
                @pl.when(n < LEADS)
                def _():
                    lead_copy(t, n, h).start()
                @pl.when(n >= LEADS)
                def _():
                    u_copy(t, n, h).start()
                    own_copy(t, n, h).start()

        @pl.when((step == GATE) & child & (x < 2))
        def _():
            for k in range(2):
                @pl.when(x == k)
                def _():
                    x_sends(1, k)
            pl.semaphore_signal(pace, inc=1, device_id=device(y, z, other, x), device_id_type=MESH)
        return 0

    @pl.when(inner & (core == 1))
    def _():
        lax.fori_loop(0, PIECES * NITEM + LAST, relay, 0)

    def lead_wait(n):
        rows = item_rows(n)
        pltpu.make_async_remote_copy(
            src_ref=buf.at[rows], dst_ref=buf.at[rows], send_sem=p_send.at[0], recv_sem=lead_recv.at[n],
            device_id=device(y, z, other, x), device_id_type=MESH).wait_recv()

    def lead_into(dst, n):
        c, k = ((0, 0), (1, 0), (1, 1))[n]
        @pl.when(root)
        def _():
            dst[0:NB, :] = ap[c, k]
        @pl.when(inner)
        def _():
            lead_wait(n)
            dst[0:NB, :] = buf[n * NB:(n + 1) * NB, :]

    def result(i, c):
        return (
            (ap.at[c, 0], ap_out.at[0]), (ap.at[c, 1], ap_out.at[1]),
            (m0.at[pl.ds(NB, NB)], fac.at[0]), (tmp, fac.at[1]), (m1.at[pl.ds(NB, NB)], fac.at[2]),
            (tmp, top), (m1.at[pl.ds(0, NB)], top),
        )[i]

    def hand(i):
        src, dst = result(i, 1)
        sem = min(i, 5)
        return pltpu.make_async_remote_copy(
            src_ref=src, dst_ref=dst, send_sem=f_send.at[sem], recv_sem=f_recv.at[sem],
            device_id=device(y, z, other, x), device_id_type=MESH)

    def keep(i):
        src, dst = result(i, 0)
        return pltpu.make_async_copy(src, dst, f_own.at[i])

    work = inner | (x < 2)

    @pl.when((core == 0) & work)
    def _():
        eye = jnp.where(
            lax.broadcasted_iota(jnp.int32, (NB, NB), 0) == lax.broadcasted_iota(jnp.int32, (NB, NB), 1), 1.0, 0.0
        ).astype(F32)
        lead_into(m0, 0)
        m0[NB:, :] = eye
        factor_tile(m0)
        inv0 = split(m0[NB:, :])
        lead_into(tmp, 1)
        l10 = dot3(split(tmp[...]), inv0, NN)
        tmp[...] = l10
        l10s = split(l10)
        lead_into(m1, 2)
        m1[0:NB, :] -= dot3(l10s, l10s, NT)
        m1[NB:, :] = eye
        for k in range(2):
            for part in range(4):
                for c in range(2):
                    fwd, _dx = x_far(k, part)
                    here = (x == k) if c == 0 else (x < 0)
                    @pl.when(jnp.logical_not(here | (x == fwd) | root))
                    def _():
                        x_wait(c, k, part)
        for i in range(4):
            hand(i).start()
            keep(i).start()
        factor_tile(m1)
        hand(4).start()
        keep(4).start()
        @pl.when(root)
        def _():
            pltpu.make_async_copy(m0.at[pl.ds(0, NB)], top, f_own.at[5]).start()
            @pl.when(x == 0)
            def _():
                hand(5).start()
            @pl.when(x != 0)
            def _():
                hand(6).start()
        for i in range(5):
            hand(i).wait_send()
            keep(i).wait()
        @pl.when(root)
        def _():
            pltpu.make_async_copy(m0.at[pl.ds(0, NB)], top, f_own.at[5]).wait()
            hand(5).wait_send()

    @pl.when((core == 0) & inner)
    def _():
        for i in range(16):
            rows = pl.ds(i * NB, NB)
            pltpu.make_async_remote_copy(
                src_ref=out.at[rows], dst_ref=out.at[rows], send_sem=p_send.at[0], recv_sem=u_recv.at[i],
                device_id=device(y, z, other, x), device_id_type=MESH).wait_recv()

    @pl.when(core == 1)
    def _():
        @pl.when(inner)
        def _():
            for i in range(16):
                pltpu.make_async_copy(
                    buf.at[pl.ds((LEADS + i) * NB, NB)], out.at[pl.ds(i * NB, NB)], out_sem.at[i]).wait()
        @pl.when(work)
        def _():
            for i in range(5):
                hand(i).wait_recv()
        @pl.when(root & work)
        def _():
            hand(5).wait_recv()

    for c in range(2):
        for k in range(2):
            for part in range(4):
                fwd, _dx = x_far(k, part)
                sender = jnp.where(root, (core == 0) & ((c, k) != (0, 1)), core == c)
                @pl.when((x == k) & sender)
                def _():
                    x_copy(c, k, part, 0, 1).wait_send()
                    x_copy(c, k, part, 1, 3).wait_send()
                if c == 1:
                    @pl.when((x == k) & (core == 1))
                    def _():
                        x_copy(c, k, part, 2, 0).wait_send()
                passed = (x == fwd) & (core == 0)
                @pl.when(passed & inner if (c, k) == (0, 1) else passed)
                def _():
                    x_copy(c, k, part, 0, 1).wait_send()

    def sent(sem, count):
        rows = pl.ds(0, count * Q)
        pltpu.make_async_remote_copy(
            src_ref=buf.at[rows], dst_ref=buf.at[rows], send_sem=sem, recv_sem=t_recv.at[0, 0],
            device_id=device(y, z, other, x), device_id_type=MESH).wait_send()

    for t in range(4):
        @pl.when(inner & (core == 1))
        def _():
            for slot, (cond, dy, dz) in enumerate(children(t, y, z)):
                @pl.when(cond)
                def _():
                    sent(t_send.at[t, slot], NITEM)
            sent(p_send.at[t], NITEM)
            @pl.when((x == 0) & firsts[t])
            def _():
                for slot in range(3):
                    sent(c_send.at[slot], 1)
        for k in range(2):
            for lead in ((2, 3) if k == 0 else (0,)):
                @pl.when(root & (core == k) & (jnp.where(x == 0, 3, 2) == lead if k == 0 else core == k))
                def _():
                    sent(t_send.at[t, 0], 8 + lead)


def front(mat):
    hb = pl.BlockSpec(memory_space=pl.ANY)
    dma = pltpu.SemaphoreType.DMA
    return pl.pallas_call(
        front_kernel,
        out_shape=(
            jax.ShapeDtypeStruct((16 * NB, NB), F32),
            jax.ShapeDtypeStruct((3, NB, NB), F32),
            jax.ShapeDtypeStruct((2, NB, NB), F32),
            jax.ShapeDtypeStruct((NB, NB), F32),
        ),
        in_specs=[hb],
        out_specs=(hb, hb, hb, hb),
        scratch_shapes=[
            pltpu.VMEM((NITEM * NB, NB), F32),
            pltpu.VMEM((2, 2, NB, NB), F32),
            pltpu.VMEM((2 * NB, NB), F32),
            pltpu.VMEM((2 * NB, NB), F32),
            pltpu.VMEM((NB, NB), F32),
            dma((9, 4)), pltpu.SemaphoreType.REGULAR, dma((3,)), dma((2, 2, 4, 3)), dma((2, 2, 4)), dma((4, 3)), dma((4, NITEM * PIECES)),
            dma((4,)), dma((LEADS,)), dma((16,)), dma((16,)), dma((6,)), dma((6,)), dma((6,)),
        ],
        compiler_params=pltpu.CompilerParams(
            collective_id=0, has_side_effects=True, vmem_limit_bytes=63 * 1024 * 1024),
    )(mat)


def tri(a, inv):
    low = tuple(v[:, :256] for v in a)
    return jnp.concatenate([
        dot3(low, tuple(v[:256, :256] for v in inv), NN),
        dot3(a, tuple(v[:, 256:] for v in inv), NN)], 1)


def tri_t(a, inv):
    high = tuple(v[:, 256:] for v in a)
    return jnp.concatenate([
        dot3(a, tuple(v[:256, :] for v in inv), NT),
        dot3(high, tuple(v[256:, 256:] for v in inv), NT)], 1)


def trail_kernel(mat, u, fac, ap, top, out, fv, av, tv, whl, sbuf, ubuf, obuf, f_sem, s_sem, u_sem, o_sem):
    x = lax.axis_index("col")
    p = lax.axis_index("row")
    OUT = obuf.shape[0]

    def s_copies(s):
        return [pltpu.make_async_copy(mat.at[:, 4 * s + b, 0, :], sbuf.at[s, :, pl.ds(128 * b, 128)], s_sem.at[s, b])
                for b in range(4)]

    def u_copy(s):
        return pltpu.make_async_copy(u.at[pl.ds(2 * s * NB, 2 * NB)], ubuf.at[s], u_sem.at[s])

    def o_copies(s):
        i = s % OUT
        return [pltpu.make_async_copy(obuf.at[i, :, pl.ds(128 * b, 128)], out.at[:, 4 * s + b, 0, :], o_sem.at[i, b])
                for b in range(4)]

    first = [
        pltpu.make_async_copy(ap.at[0], av.at[0], f_sem.at[0]),
        pltpu.make_async_copy(fac.at[0], fv.at[0], f_sem.at[1]),
        pltpu.make_async_copy(ap.at[1], av.at[1], f_sem.at[2]),
        pltpu.make_async_copy(fac.at[1], fv.at[1], f_sem.at[3]),
        pltpu.make_async_copy(fac.at[2], fv.at[2], f_sem.at[4]),
        pltpu.make_async_copy(top, tv, f_sem.at[5]),
    ]
    for cp in first:
        cp.start()
    for s in range(8):
        u_copy(s).start()
        for cp in s_copies(s):
            cp.start()

    first[0].wait()
    first[1].wait()
    inv0 = split(fv[0])
    x0 = tri(split(av[0]), inv0)
    first[2].wait()
    first[3].wait()
    l10 = split(fv[1])
    rest = av[1] - dot3(split(x0), l10, NT)
    first[4].wait()
    inv1 = split(fv[2])
    x1 = tri(split(rest), inv1)
    v = tri_t(split(x1), inv1)
    vs = split(v)
    ws = split(tri_t(split(x0 - dot3(vs, l10, NN)), inv0))
    for i in range(2):
        whl[i, :, :NB] = ws[i]
        whl[i, :, NB:] = vs[i]
    first[5].wait()
    own = jnp.where((p == 0) & (x > 0), 0.0, tv[...])
    av[0] = jnp.where(p < 2, own, jnp.where(x == 0, x0, x1))

    for s in range(8):
        if s >= OUT:
            for cp in o_copies(s - OUT):
                cp.wait()
        u_copy(s).wait()
        for cp in s_copies(s):
            cp.wait()
        for h in range(2):
            cols = pl.ds(256 * h, 256)
            part = split(ubuf[s, :, cols])
            new = sbuf[s, :, cols] - dot3((whl[0], whl[1]), part, NN)
            new = jnp.where(p < 2, 0.0, new)
            if s == 0:
                new = jnp.where(x < 2, av[0, :, cols], new)
            obuf[s % OUT, :, cols] = new
        for cp in o_copies(s):
            cp.start()
    for s in range(8 - OUT, 8):
        for cp in o_copies(s):
            cp.wait()


def trail(mat, u, fac, ap, top):
    hb = pl.BlockSpec(memory_space=pl.ANY)
    dma = pltpu.SemaphoreType.DMA
    return pl.pallas_call(
        trail_kernel,
        out_shape=jax.ShapeDtypeStruct(mat.shape, F32),
        in_specs=[hb] * 5,
        out_specs=hb,
        scratch_shapes=[
            pltpu.VMEM((3, NB, NB), F32), pltpu.VMEM((2, NB, NB), F32), pltpu.VMEM((NB, NB), F32),
            pltpu.VMEM((2, NB, 2 * NB), BF),
            pltpu.VMEM((8, NB, NB), F32), pltpu.VMEM((8, 2 * NB, NB), F32), pltpu.VMEM((3, NB, NB), F32),
            dma((6,)), dma((8, 4)), dma((8,)), dma((3, 4)),
        ],
        compiler_params=pltpu.CompilerParams(vmem_limit_bytes=63 * 1024 * 1024),
    )(mat, u, fac, ap, top)


def shards(matrix):
    mat = matrix.reshape(NB, 32, 1, 128)
    return trail(mat, *front(mat)).reshape(matrix.shape)


def solution(mesh):
    spec = P(None, "row", None, None, "col", None)
    return jax.shard_map(shards, mesh=mesh, in_specs=(spec,), out_specs=spec, check_vma=False)
```

```python
import functools
import jax
import jax.numpy as jnp
from jax import lax
from jax.experimental import pallas as pl
from jax.experimental.pallas import tpu as pltpu
from jax.sharding import PartitionSpec as P

F32 = jnp.float32
BF = jnp.bfloat16
MESH = pl.DeviceIdType.MESH
NT = (((1,), (1,)), ((), ()))
NN = (((1,), (0,)), ((), ()))
NB = 512
Q = 128


def split(x):
    h=x.astype(BF)
    return h,(x-h.astype(F32)).astype(BF)

def dot3(a,b,dims):
    ah,al=a; bh,bl=b
    d=functools.partial(lax.dot_general,dimension_numbers=dims,preferred_element_type=F32)
    return d(ah,bh)+d(ah,bl)+d(al,bh)

def factor128(D):
    D3 = [D[8 * i:8 * i + 8, :] for i in range(16)]
    lane = lax.broadcasted_iota(jnp.int32, (8, 128), 1)
    sub = lax.broadcasted_iota(jnp.int32, (8, 128), 0)
    E3 = [jnp.where(lane == sub + 8 * i, 1.0, 0.0).astype(F32) for i in range(16)]
    zero = jnp.zeros((8, 128), F32)

    def bs(x, k):
        return jnp.take_along_axis(x, jnp.full((8, 128), k, jnp.int32), axis=0)

    U = [None] * 16
    for b in range(16):
        c = 8 * b
        B = {}
        for i in range(b, 16):
            for k in range(8):
                B[i, k] = jnp.broadcast_to(D3[i][:, c + k:c + k + 1], (8, 128))
        g = {(k, m): bs(B[b, m], k) for m in range(8) for k in range(m, 8)}
        r = [None] * 8
        s = {}
        for m in range(8):
            r[m] = lax.rsqrt(g[m, m])
            for k in range(m + 1, 8):
                s[k, m] = g[k, m] * r[m]
            for l in range(m + 1, 8):
                for k in range(l, 8):
                    g[k, l] = g[k, l] - s[k, m] * s[l, m]
        urow, erow = [], []
        for i in range(b, 16):
            mk = []
            for k in range(8):
                v = B[i, k]
                for m in range(k):
                    v = v - mk[m] * s[k, m]
                mk.append(v * r[k])
            d, e = D3[i], E3[i]
            if i == b:
                ou, oe = zero, zero
                for k in range(8):
                    u, w = bs(d, k) * r[k], bs(e, k) * r[k]
                    urow.append(u)
                    erow.append(w)
                    ou, oe = jnp.where(sub == k, u, ou), jnp.where(sub == k, w, oe)
                    if k < 7:
                        mm = jnp.where(sub > k, mk[k], 0.0)
                        d, e = d - mm * u, e - mm * w
                U[b] = jnp.where(lane >= sub + c, ou, 0.0)
                E3[b] = oe
            else:
                for k in range(8):
                    d, e = d - mk[k] * urow[k], e - mk[k] * erow[k]
                D3[i], E3[i] = d, e
    return jnp.concatenate(U, 0), jnp.concatenate(E3, 0)


def factor_tile(M):
    row = lax.broadcasted_iota(jnp.int32, (512, 128), 0)

    def body(k, _):
        c0 = pl.multiple_of(k * 128, 128)
        cols = pl.ds(c0, 128)
        U, Linv = factor128(M[cols, cols])
        live = pl.ds(pl.multiple_of(c0 + 128, 128), 512)
        X = dot3(split(M[live, cols]), split(Linv), NT)
        M[live, cols] = X
        M[cols, cols] = U.T
        below = M[0:512, cols]
        M[0:512, cols] = jnp.where(row >= c0, below, 0.0)
        xs = split(X)
        for j in range(3):
            @pl.when(k == j)
            def _():
                right = slice(128 * (j + 1), 512)
                lead = split(below[right])
                for h in range(2):
                    r = slice(256 * h, 256 * h + 256)
                    start = 128 * (j + 1) + 256 * h
                    M[start:start + 256, right] -= dot3(tuple(v[r] for v in xs), lead, NT)
        return 0

    lax.fori_loop(0, 4, body, 0)

LEADS = 3
NITEM = LEADS + 16
EVEN = [3, 5, 7, 1, 2, 9, 11, 13, 15, 17]
ODD = [4, 6, 8, 10, 12, 14, 16, 18]
DEEP = 6
PIECES = 4
GATE = 12
R = Q // PIECES


def place():
    row = lax.axis_index("row")
    return lax.rem(row, 2), lax.rem(row // 2, 4), row // 8, lax.axis_index("col")


def device(y, z, core, x):
    return ((lax.rem(z + 4, 4) * 4 + lax.rem(y + 4, 4)) * 2 + core, lax.rem(x + 4, 4))


def to_tree(t, y, z):
    if t == 0:
        return y, z
    if t == 1:
        return lax.rem(4 - y, 4), lax.rem(4 - z, 4)
    if t == 2:
        return z, y
    return lax.rem(4 - z, 4), lax.rem(4 - y, 4)


def depth(t, y, z):
    u, v = to_tree(t, y, z)
    return jnp.where((u == 0) & (v > 0), 2 + v, u + v)


def at_step(i, x):
    j = i // 2
    at = jnp.where(x == 0, 0, 1)
    even = jnp.where(j < 2, jnp.where(j == at, 0, 3), jnp.where(j < 4, 2 * j + 1, jnp.where(j < 6, j - 3, 2 * j - 3)))
    return jnp.where(i >= 16, 13 + 2 * (i - 16), jnp.where(lax.rem(i, 2) == 1, 4 + 2 * j, even))


def children(t, y, z):
    u, v = to_tree(t, y, z)
    steps = {0: ((1, 0), (0, 1)), 1: ((-1, 0), (0, -1)), 2: ((0, 1), (1, 0)), 3: ((0, -1), (-1, 0))}
    (uy, uz), (vy, vz) = steps[t]
    return (
        ((v == 0) & (u < 3), uy, uz),
        ((u >= 1) & (v < 3), vy, vz),
        ((u == 1) & (v >= 1), -uy, -uz),
    )


def front_kernel(mat, out, fac, ap_out, top, buf, ap, m0, m1, tmp,
                 load_sem, pace, c_send, x_send, x_recv, t_send, t_recv, p_send, lead_recv, u_recv, out_sem, f_send, f_recv, f_own):
    core, y, z, x = place()
    root = (y == 0) & (z == 0)
    inner = jnp.logical_not(root)
    firsts = [depth(t, y, z) == 1 for t in range(4)]
    child = firsts[0] | firsts[1] | firsts[2] | firsts[3]
    other = 1 - core

    def tile_load(s, dst, sem):
        return [
            pltpu.make_async_copy(mat.at[:, 4 * s + b, 0, :], dst.at[:, pl.ds(128 * b, 128)], sem.at[b])
            for b in range(4)
        ]

    def item_rows(n):
        return pl.ds(n * NB, NB)

    def item(k, s):
        return LEADS + 2 * s + k

    for k in range(2):
        for c in range(2):
            @pl.when((x == k) & (core == c))
            def _():
                for cp in tile_load(0, ap.at[c, k], load_sem.at[8]):
                    cp.start()
    def row_loads(tiles):
        for k in range(2):
            @pl.when(root & (core == k))
            def _():
                for s in tiles:
                    for cp in tile_load(s, buf.at[item_rows(item(k, s))], load_sem.at[s]):
                        cp.start()

    row_loads((0,))

    barrier = pltpu.get_barrier_semaphore()
    peers = [device(y, z, other, x)]
    for c in range(2):
        peers += [device(y, z, c, x + d) for d in (1, 2, 3)]
        for dy, dz in ((1, 0), (3, 0), (0, 1), (0, 3)):
            peers.append(device(y + dy, z + dz, c, x))
    for peer in peers:
        pl.semaphore_signal(barrier, inc=1, device_id=peer, device_id_type=MESH)
    pl.semaphore_wait(barrier, len(peers))
    row_loads(range(1, 8))

    def x_copy(c, k, part, slot, dx):
        rows = pl.ds(Q * part, Q)
        return pltpu.make_async_remote_copy(
            src_ref=ap.at[c, k, rows], dst_ref=ap.at[c, k, rows],
            send_sem=x_send.at[c, k, part, slot], recv_sem=x_recv.at[c, k, part],
            device_id=device(y, z, 0, x + dx), device_id_type=MESH)

    def x_sends(c, k):
        for part in range(4):
            x_copy(c, k, part, 0, 1).start()
            x_copy(c, k, 3 - part, 1, 3).start()

    for k in range(2):
        for c in range(2):
            @pl.when((x == k) & (core == c))
            def _():
                for cp in tile_load(0, ap.at[c, k], load_sem.at[8]):
                    cp.wait()
                if c == 1:
                    for part in range(4):
                        x_copy(c, k, part, 2, 0).start()
                away = inner & jnp.logical_not(child)
                @pl.when(away)
                def _():
                    x_sends(c, k)

    def x_far(k, part):
        return lax.rem(k + (1 if part < 2 else 3), 4), (1 if part < 2 else 3)

    def x_wait(c, k, part):
        x_copy(c, k, part, 0, 1).wait_recv()

    def x_forward(c, k):
        for part in (0, 3, 1, 2):
            fwd, dx = x_far(k, part)
            @pl.when(x == fwd)
            def _():
                x_wait(c, k, part)
                x_copy(c, k, part, 0, dx).start()

    def root_send(k):
        @pl.when(x == k)
        def _():
            for part in range(4):
                x_wait(1, k, part)
            x_sends(1, k)

    def root_rest(c, k, part):
        fwd, _dx = x_far(k, part)
        @pl.when((x != k) & (x != fwd))
        def _():
            x_wait(c, k, part)

    def piece(t, n, h):
        return pl.ds(pl.multiple_of(n * NB + t * Q + h * R, 8), R)

    def tree_copy(t, n, h, slot, dy, dz, src=None):
        rows = piece(t, n, h)
        return pltpu.make_async_remote_copy(
            src_ref=buf.at[rows] if src is None else src.at[pl.ds(t * Q + h * R, R)],
            dst_ref=buf.at[rows],
            send_sem=t_send.at[t, slot], recv_sem=t_recv.at[t, n * PIECES + h],
            device_id=device(y + dy, z + dz, 1, x), device_id_type=MESH)

    def lead_copy(t, n, h):
        rows = piece(t, n, h)
        return pltpu.make_async_remote_copy(
            src_ref=buf.at[rows], dst_ref=buf.at[rows],
            send_sem=p_send.at[t], recv_sem=lead_recv.at[n],
            device_id=device(y, z, other, x), device_id_type=MESH)

    def out_piece(t, n, h):
        return pl.ds(pl.multiple_of((n - LEADS) * NB + t * Q + h * R, 8), R)

    def u_copy(t, n, h):
        return pltpu.make_async_remote_copy(
            src_ref=buf.at[piece(t, n, h)], dst_ref=out.at[out_piece(t, n, h)],
            send_sem=p_send.at[t], recv_sem=u_recv.at[n - LEADS],
            device_id=device(y, z, other, x), device_id_type=MESH)

    def own_copy(t, n, h):
        return pltpu.make_async_copy(buf.at[piece(t, n, h)], out.at[out_piece(t, n, h)], out_sem.at[n - LEADS])

    def root_tree(n, src):
        for t in range(4):
            (_, dy, dz), _b, _c = children(t, y, z)
            for h in range(PIECES):
                tree_copy(t, n, h, 0, dy, dz, src).start()

    @pl.when(root & (core == 0))
    def _():
        @pl.when(x == 0)
        def _():
            root_tree(0, ap.at[0, 0])
        for k in range(2):
            root_send(k)
        @pl.when(x == 0)
        def _():
            for part in range(4):
                x_copy(0, 0, part, 0, 1).start()
        for n in EVEN:
            if n < LEADS:
                kk = n - 1
                if n == 1:
                    x_forward(1, 0)
                    x_forward(1, 1)
                for t in range(4):
                    root_rest(1, kk, t)
                root_tree(n, ap.at[1, kk])
            else:
                for cp in tile_load((n - LEADS) // 2, buf.at[item_rows(n)], load_sem.at[(n - LEADS) // 2]):
                    cp.wait()
                root_tree(n, None)
            if n in EVEN[:7]:
                pl.semaphore_signal(pace, inc=1, device_id=device(y, z, other, x), device_id_type=MESH)
        @pl.when(x == 1)
        def _():
            for part in range(4):
                x_wait(0, 0, part)

    @pl.when(root & (core == 1))
    def _():
        for n in ODD:
            for cp in tile_load((n - LEADS) // 2, buf.at[item_rows(n)], load_sem.at[(n - LEADS) // 2]):
                cp.wait()
            if n > 4:
                pl.semaphore_wait(pace, 1)
            root_tree(n, None)

    def cross_copy(t, h, slot):
        rows = piece(t, 0, h)
        return pltpu.make_async_remote_copy(
            src_ref=buf.at[rows], dst_ref=buf.at[rows],
            send_sem=c_send.at[slot], recv_sem=t_recv.at[t, h],
            device_id=device(y, z, 1, x + slot + 1), device_id_type=MESH)

    @pl.when(child & (core == 0) & (x < 2))
    def _():
        pl.semaphore_wait(pace, 1)
        for k in range(2):
            @pl.when(x == k)
            def _():
                x_sends(0, k)

    @pl.when(inner & (core == 0))
    def _():
        for k in range(2):
            for c in range(2):
                x_forward(c, k)

    skews = [4 * depth(t, y, z) for t in range(4)]
    LAST = 4 * DEEP

    def relay(step, _):
        for t in range(4):
            i = step - skews[t]
            @pl.when((i >= 0) & (i < PIECES * NITEM))
            def _():
                n, h = at_step(i // PIECES, x), lax.rem(i, PIECES)
                tree_copy(t, n, h, 0, 0, 1).wait_recv()
                for slot, (cond, dy, dz) in enumerate(children(t, y, z)):
                    @pl.when(cond)
                    def _():
                        tree_copy(t, n, h, slot, dy, dz).start()
                @pl.when((n == 0) & (x == 0) & firsts[t])
                def _():
                    for slot in (0, 2, 1):
                        cross_copy(t, h, slot).start()
                @pl.when(n < LEADS)
                def _():
                    lead_copy(t, n, h).start()
                @pl.when(n >= LEADS)
                def _():
                    u_copy(t, n, h).start()
                    own_copy(t, n, h).start()

        @pl.when((step == GATE) & child & (x < 2))
        def _():
            for k in range(2):
                @pl.when(x == k)
                def _():
                    x_sends(1, k)
            pl.semaphore_signal(pace, inc=1, device_id=device(y, z, other, x), device_id_type=MESH)
        return 0

    @pl.when(inner & (core == 1))
    def _():
        lax.fori_loop(0, PIECES * NITEM + LAST, relay, 0)

    def lead_wait(n):
        rows = item_rows(n)
        pltpu.make_async_remote_copy(
            src_ref=buf.at[rows], dst_ref=buf.at[rows], send_sem=p_send.at[0], recv_sem=lead_recv.at[n],
            device_id=device(y, z, other, x), device_id_type=MESH).wait_recv()

    def lead_into(dst, n):
        c, k = ((0, 0), (1, 0), (1, 1))[n]
        @pl.when(root)
        def _():
            dst[0:NB, :] = ap[c, k]
        @pl.when(inner)
        def _():
            lead_wait(n)
            dst[0:NB, :] = buf[n * NB:(n + 1) * NB, :]

    def result(i, c):
        return (
            (ap.at[c, 0], ap_out.at[0]), (ap.at[c, 1], ap_out.at[1]),
            (m0.at[pl.ds(NB, NB)], fac.at[0]), (tmp, fac.at[1]), (m1.at[pl.ds(NB, NB)], fac.at[2]),
            (tmp, top), (m1.at[pl.ds(0, NB)], top),
        )[i]

    def hand(i):
        src, dst = result(i, 1)
        sem = min(i, 5)
        return pltpu.make_async_remote_copy(
            src_ref=src, dst_ref=dst, send_sem=f_send.at[sem], recv_sem=f_recv.at[sem],
            device_id=device(y, z, other, x), device_id_type=MESH)

    def keep(i):
        src, dst = result(i, 0)
        return pltpu.make_async_copy(src, dst, f_own.at[i])

    work = inner | (x < 2)

    @pl.when((core == 0) & work)
    def _():
        eye = jnp.where(
            lax.broadcasted_iota(jnp.int32, (NB, NB), 0) == lax.broadcasted_iota(jnp.int32, (NB, NB), 1), 1.0, 0.0
        ).astype(F32)
        lead_into(m0, 0)
        m0[NB:, :] = eye
        factor_tile(m0)
        inv0 = split(m0[NB:, :])
        lead_into(tmp, 1)
        l10 = dot3(split(tmp[...]), inv0, NN)
        tmp[...] = l10
        l10s = split(l10)
        lead_into(m1, 2)
        m1[0:NB, :] -= dot3(l10s, l10s, NT)
        m1[NB:, :] = eye
        for k in range(2):
            for part in range(4):
                for c in range(2):
                    fwd, _dx = x_far(k, part)
                    here = (x == k) if c == 0 else (x < 0)
                    @pl.when(jnp.logical_not(here | (x == fwd) | root))
                    def _():
                        x_wait(c, k, part)
        for i in range(4):
            hand(i).start()
            keep(i).start()
        factor_tile(m1)
        hand(4).start()
        keep(4).start()
        @pl.when(root)
        def _():
            pltpu.make_async_copy(m0.at[pl.ds(0, NB)], top, f_own.at[5]).start()
            @pl.when(x == 0)
            def _():
                hand(5).start()
            @pl.when(x != 0)
            def _():
                hand(6).start()
        for i in range(5):
            hand(i).wait_send()
            keep(i).wait()
        @pl.when(root)
        def _():
            pltpu.make_async_copy(m0.at[pl.ds(0, NB)], top, f_own.at[5]).wait()
            hand(5).wait_send()

    @pl.when((core == 0) & inner)
    def _():
        for i in range(16):
            rows = pl.ds(i * NB, NB)
            pltpu.make_async_remote_copy(
                src_ref=out.at[rows], dst_ref=out.at[rows], send_sem=p_send.at[0], recv_sem=u_recv.at[i],
                device_id=device(y, z, other, x), device_id_type=MESH).wait_recv()

    @pl.when(core == 1)
    def _():
        @pl.when(inner)
        def _():
            for i in range(16):
                pltpu.make_async_copy(
                    buf.at[pl.ds((LEADS + i) * NB, NB)], out.at[pl.ds(i * NB, NB)], out_sem.at[i]).wait()
        @pl.when(work)
        def _():
            for i in range(5):
                hand(i).wait_recv()
        @pl.when(root & work)
        def _():
            hand(5).wait_recv()

    for c in range(2):
        for k in range(2):
            for part in range(4):
                fwd, _dx = x_far(k, part)
                sender = jnp.where(root, (core == 0) & ((c, k) != (0, 1)), core == c)
                @pl.when((x == k) & sender)
                def _():
                    x_copy(c, k, part, 0, 1).wait_send()
                    @pl.when(inner if (c, k) == (0, 0) else x == k)
                    def _():
                        x_copy(c, k, part, 1, 3).wait_send()
                if c == 1:
                    @pl.when((x == k) & (core == 1))
                    def _():
                        x_copy(c, k, part, 2, 0).wait_send()
                passed = (x == fwd) & (core == 0)
                @pl.when(passed & inner if c == 0 else passed)
                def _():
                    x_copy(c, k, part, 0, 1).wait_send()

    def sent(sem, count):
        rows = pl.ds(0, count * Q)
        pltpu.make_async_remote_copy(
            src_ref=buf.at[rows], dst_ref=buf.at[rows], send_sem=sem, recv_sem=t_recv.at[0, 0],
            device_id=device(y, z, other, x), device_id_type=MESH).wait_send()

    for t in range(4):
        @pl.when(inner & (core == 1))
        def _():
            for slot, (cond, dy, dz) in enumerate(children(t, y, z)):
                @pl.when(cond)
                def _():
                    sent(t_send.at[t, slot], NITEM)
            sent(p_send.at[t], NITEM)
            @pl.when((x == 0) & firsts[t])
            def _():
                for slot in range(3):
                    sent(c_send.at[slot], 1)
        for k in range(2):
            for lead in ((2, 3) if k == 0 else (0,)):
                @pl.when(root & (core == k) & (jnp.where(x == 0, 3, 2) == lead if k == 0 else core == k))
                def _():
                    sent(t_send.at[t, 0], 8 + lead)


def front(mat):
    hb = pl.BlockSpec(memory_space=pl.ANY)
    dma = pltpu.SemaphoreType.DMA
    return pl.pallas_call(
        front_kernel,
        out_shape=(
            jax.ShapeDtypeStruct((16 * NB, NB), F32),
            jax.ShapeDtypeStruct((3, NB, NB), F32),
            jax.ShapeDtypeStruct((2, NB, NB), F32),
            jax.ShapeDtypeStruct((NB, NB), F32),
        ),
        in_specs=[hb],
        out_specs=(hb, hb, hb, hb),
        scratch_shapes=[
            pltpu.VMEM((NITEM * NB, NB), F32),
            pltpu.VMEM((2, 2, NB, NB), F32),
            pltpu.VMEM((2 * NB, NB), F32),
            pltpu.VMEM((2 * NB, NB), F32),
            pltpu.VMEM((NB, NB), F32),
            dma((9, 4)), pltpu.SemaphoreType.REGULAR, dma((3,)), dma((2, 2, 4, 3)), dma((2, 2, 4)), dma((4, 3)), dma((4, NITEM * PIECES)),
            dma((4,)), dma((LEADS,)), dma((16,)), dma((16,)), dma((6,)), dma((6,)), dma((6,)),
        ],
        compiler_params=pltpu.CompilerParams(
            collective_id=0, has_side_effects=True, vmem_limit_bytes=63 * 1024 * 1024),
    )(mat)


def tri(a, inv):
    low = tuple(v[:, :256] for v in a)
    return jnp.concatenate([
        dot3(low, tuple(v[:256, :256] for v in inv), NN),
        dot3(a, tuple(v[:, 256:] for v in inv), NN)], 1)


def tri_t(a, inv):
    high = tuple(v[:, 256:] for v in a)
    return jnp.concatenate([
        dot3(a, tuple(v[:256, :] for v in inv), NT),
        dot3(high, tuple(v[256:, 256:] for v in inv), NT)], 1)


def trail_kernel(mat, u, fac, ap, top, out, fv, av, tv, whl, sbuf, ubuf, obuf, f_sem, s_sem, u_sem, o_sem):
    x = lax.axis_index("col")
    p = lax.axis_index("row")
    OUT = obuf.shape[0]

    def s_copies(s):
        return [pltpu.make_async_copy(mat.at[:, 4 * s + b, 0, :], sbuf.at[s, :, pl.ds(128 * b, 128)], s_sem.at[s, b])
                for b in range(4)]

    def u_copy(s):
        return pltpu.make_async_copy(u.at[pl.ds(2 * s * NB, 2 * NB)], ubuf.at[s], u_sem.at[s])

    def o_copies(s):
        i = s % OUT
        return [pltpu.make_async_copy(obuf.at[i, :, pl.ds(128 * b, 128)], out.at[:, 4 * s + b, 0, :], o_sem.at[i, b])
                for b in range(4)]

    first = [
        pltpu.make_async_copy(ap.at[0], av.at[0], f_sem.at[0]),
        pltpu.make_async_copy(fac.at[0], fv.at[0], f_sem.at[1]),
        pltpu.make_async_copy(ap.at[1], av.at[1], f_sem.at[2]),
        pltpu.make_async_copy(fac.at[1], fv.at[1], f_sem.at[3]),
        pltpu.make_async_copy(fac.at[2], fv.at[2], f_sem.at[4]),
        pltpu.make_async_copy(top, tv, f_sem.at[5]),
    ]
    for cp in first:
        cp.start()
    def load(tiles):
        for s in tiles:
            u_copy(s).start()
            for cp in s_copies(s):
                cp.start()

    first[0].wait()
    first[1].wait()
    inv0 = split(fv[0])
    x0 = tri(split(av[0]), inv0)
    first[2].wait()
    first[3].wait()
    l10 = split(fv[1])
    rest = av[1] - dot3(split(x0), l10, NT)
    first[4].wait()
    load(range(8))
    inv1 = split(fv[2])
    x1 = tri(split(rest), inv1)
    v = tri_t(split(x1), inv1)
    vs = split(v)
    ws = split(tri_t(split(x0 - dot3(vs, l10, NN)), inv0))
    for i, h in enumerate((0, 0, 1)):
        whl[:, 2 * NB * i:2 * NB * i + NB] = ws[h]
        whl[:, 2 * NB * i + NB:2 * NB * (i + 1)] = vs[h]
    first[5].wait()
    own = jnp.where((p == 0) & (x > 0), 0.0, tv[...])
    av[0] = jnp.where(p < 2, own, jnp.where(x == 0, x0, x1))

    for s in range(8):
        if s >= OUT:
            for cp in o_copies(s - OUT):
                cp.wait()
        u_copy(s).wait()
        for cp in s_copies(s):
            cp.wait()
        for h in range(2):
            cols = pl.ds(256 * h, 256)
            uh, ul = split(ubuf[s, :, cols])
            part = jnp.concatenate([uh, ul, uh], 0)
            new = sbuf[s, :, cols] - lax.dot_general(whl[...], part, NN, preferred_element_type=F32)
            new = jnp.where(p < 2, 0.0, new)
            if s == 0:
                new = jnp.where(x < 2, av[0, :, cols], new)
            obuf[s % OUT, :, cols] = new
        for cp in o_copies(s):
            cp.start()
    for s in range(8 - OUT, 8):
        for cp in o_copies(s):
            cp.wait()


def trail(mat, u, fac, ap, top):
    hb = pl.BlockSpec(memory_space=pl.ANY)
    dma = pltpu.SemaphoreType.DMA
    return pl.pallas_call(
        trail_kernel,
        out_shape=jax.ShapeDtypeStruct(mat.shape, F32),
        in_specs=[hb] * 5,
        out_specs=hb,
        scratch_shapes=[
            pltpu.VMEM((3, NB, NB), F32), pltpu.VMEM((2, NB, NB), F32), pltpu.VMEM((NB, NB), F32),
            pltpu.VMEM((NB, 6 * NB), BF),
            pltpu.VMEM((8, NB, NB), F32), pltpu.VMEM((8, 2 * NB, NB), F32), pltpu.VMEM((3, NB, NB), F32),
            dma((6,)), dma((8, 4)), dma((8,)), dma((3, 4)),
        ],
        compiler_params=pltpu.CompilerParams(vmem_limit_bytes=63 * 1024 * 1024),
    )(mat, u, fac, ap, top)


def shards(matrix):
    mat = matrix.reshape(NB, 32, 1, 128)
    return trail(mat, *front(mat)).reshape(matrix.shape)


def solution(mesh):
    spec = P(None, "row", None, None, "col", None)
    return jax.shard_map(shards, mesh=mesh, in_specs=(spec,), out_specs=spec, check_vma=False)
```
